256 devices in a mesh: band: 32 (over y, x, core), gslab: 8 (over z).
Axes of the slice: x: 4, y: 4, z: 8, core: 2. Of those that a mesh axis runs over, the one named last changes fastest.
Arguments:
- band_coeffs: float32 [12288, 49152], P('band', 'gslab'), may hold values from -6 to 6
- sign_table: int32 [12, 12288], P(None, 'band'), may hold values from -1 to 1, as said below
- slice_widths: int32 [64], replicated, may hold values from 96 to 384, as said below
- owner_map: int32 [64], replicated, may hold values from 0 to 63, each once
Outputs:
- pseudobands: float32 [768, 49152], P(('band', 'gslab'))
The draws below stay inside these ranges and needn't reach their ends.
Inputs may be any that keep to these rules, and one draw needn't show every extreme that they name: `sign_table`: every entry is -1 or 1. `slice_widths`: the widths sum to 12288; every slice holds 96 to 384 bands, and in every draw some slice holds exactly 96 and some exactly 384. `owner_map`: each slice appears once.
All inputs are finite; a program needn't handle non-finite values.
Results may differ from the reference program's by a relative error of at most 0.0003.
Values sent between devices are 32-bit elements; how exact they have to be, the bound alone decides.
A program may use at most 128 MiB of HBM per device.

```python
import jax
import jax.numpy as jnp
from jax import lax

NG = 49152
BANDS_DEV = 384
SLICE_BAND = 2
NPS = 12
NB = 12288
NSLICE = 64
MOST = 384
NPB = 768


def draw_sign_table(key, part):
    return (2 * jax.random.randint(jax.random.fold_in(key, 17), (NPS, NB), 0, 2) - 1).astype(jnp.int32)


def draw_slice_widths(key, part):
    average = BANDS_DEV // SLICE_BAND
    narrow = average // 2
    place = jax.random.randint(jax.random.fold_in(key, 3), (), 0, NSLICE - 3)
    positions = jnp.arange(NSLICE, dtype=jnp.int32)
    relative = positions - place
    special = (relative >= 0) & (relative < 4)
    ranking = jnp.where(positions < place, positions, positions - 4)
    ranking = jnp.maximum(ranking, 0)
    pair_id = jnp.minimum(ranking // 2, NSLICE // 2 - 1)
    parity = ranking % 2
    spread = jax.random.randint(jax.random.fold_in(key, 5), (NSLICE // 2,), -(average - narrow), average - narrow + 1)
    shift_value = spread[pair_id]
    drawn = average + jnp.where(parity == 0, shift_value, -shift_value)
    table = jnp.array([narrow, 2 * average, narrow, average], dtype=jnp.int32)
    marked = table[jnp.clip(relative, 0, 3)]
    return jnp.where(special, marked, drawn).astype(jnp.int32)


def block_levels(key, extent, split, low, largest):
    level, own = 1.0, jax.random.fold_in(key, 6)
    for position, blocks in split:
        draws = jnp.exp(jax.random.uniform(jax.random.fold_in(own, position), (blocks,), jnp.float32, low / len(split), largest / len(split)))
        level = level * jnp.repeat(draws, extent[position] // blocks).reshape([-1 if axis == position else 1 for axis in range(len(extent))])
    return level


def centred(rng, shape, width, most, split=(), kind=jnp.bfloat16):
    values = width * jax.random.normal(rng, shape, jnp.float32)
    if split:
        values = values * block_levels(rng, shape, split, -0.22, 0.18)
    return jnp.clip(values, -most, most).astype(kind)


def setup_inputs(seed: int = 0) -> dict:
    key_of = jax.random.split(jax.random.key(seed), 5)
    return {
        "band_coeffs": centred(key_of[0], (NB, NG), 1.0, 6.0, ((0, 32), (1, 8)), jnp.float32),
        "sign_table": draw_sign_table(jax.random.fold_in(key_of[4], 71), 0),
        "slice_widths": draw_slice_widths(jax.random.fold_in(key_of[4], 71), 0),
        "owner_map": jax.random.permutation(key_of[3], NSLICE).astype(jnp.int32),
    }


def reference(band_coeffs, sign_table, slice_widths, owner_map):
    ends = jnp.cumsum(slice_widths).astype(jnp.int32)
    starts = (ends - slice_widths).astype(jnp.int32)
    inverse = 1.0 / jnp.sqrt(slice_widths.astype(jnp.float32))

    def one_slice(slice_id):
        begin = starts[slice_id]
        finish = ends[slice_id]
        window_start = jnp.minimum(begin, NB - MOST).astype(jnp.int32)
        block = lax.dynamic_slice(band_coeffs, (window_start, jnp.int32(0)), (MOST, NG))
        band_ids = window_start + jnp.arange(MOST, dtype=jnp.int32)
        inside = (band_ids >= begin) & (band_ids < finish)
        sign_block = lax.dynamic_slice(sign_table, (jnp.int32(0), window_start), (NPS, MOST)).astype(jnp.float32)
        weights = jnp.where(inside[None, :], sign_block * inverse[slice_id], jnp.zeros_like(sign_block))
        return jnp.dot(weights, block, precision=lax.Precision.HIGHEST, preferred_element_type=jnp.float32)
    result = lax.map(one_slice, jnp.arange(NSLICE, dtype=jnp.int32))
    return result[owner_map].reshape(NPB, NG)
```

```python
import jax
import jax.numpy as jnp
from jax import lax
from jax.experimental import pallas as pl
from jax.experimental.pallas import tpu as pltpu
from jax.sharding import PartitionSpec as P

MESH = pl.DeviceIdType.MESH
F32 = jnp.float32
BF16 = jnp.bfloat16

NX, NY, NZ = 4, 4, 8
CHIPS = NX * NY
GROUPS = 2 * CHIPS
BANDS = 384
SLAB = 6144
PHASES = 3
WIDE = SLAB // PHASES
NPS = 12
HALF = 6
SLOTS = 5
ROWS = 32
NSLICE = 64
OUT = NSLICE * HALF

OFFSETS = (
    (1, 0), (0, 1), (3, 0), (0, 3), (1, 1), (3, 3), (1, 3), (3, 1),
    (2, 0), (0, 2), (2, 1), (1, 2), (2, 3), (3, 2), (2, 2),
)


def iota(shape, dim):
    return lax.broadcasted_iota(jnp.int32, shape, dim)


def kernel(
    band_ref, sign_ref, width_ref, owner_ref, out_ref,
    coeffs, sign, width, owner, select, scale,
    a_send, a_recv, z_send, z_recv,
    load_sem, small_sem, a_ssem, a_rsem, z_ssem, z_rsem, b_ssem, b_rsem,
):
    b = lax.axis_index("band")
    g = lax.axis_index("gslab")
    c = lax.rem(b, 2)
    q = b // 2
    x = lax.rem(q, NX)
    y = q // NX

    def chip_at(dx, dy):
        return lax.rem(y + dy, NY) * NX + lax.rem(x + dx, NX)

    loads = [
        pltpu.make_async_copy(band_ref.at[:, pl.ds(p * WIDE, WIDE)], coeffs.at[p], load_sem.at[p])
        for p in range(PHASES)
    ]
    smalls = [
        pltpu.make_async_copy(src, dst, small_sem.at[i])
        for i, (src, dst) in enumerate(((sign_ref, sign), (width_ref, width), (owner_ref, owner)))
    ]
    for copy in smalls:
        copy.start()
    for copy in loads:
        copy.start()

    barrier = pltpu.get_barrier_semaphore()
    greeted = 0
    for dc in range(2):
        for dx, dy in ((0, 0),) + OFFSETS:
            if (dc, dx, dy) != (0, 0, 0):
                peer = chip_at(dx, dy) * 2 + lax.rem(c + dc, 2)
                pl.semaphore_signal(barrier, inc=1, device_id=(peer, g), device_id_type=MESH)
                greeted += 1
        for dz in range(1, NZ):
            peer = q * 2 + lax.rem(c + dc, 2)
            pl.semaphore_signal(
                barrier, inc=1, device_id=(peer, lax.rem(g + dz, NZ)), device_id_type=MESH
            )
            greeted += 1

    for copy in smalls:
        copy.wait()
    width_row = width[...].astype(F32)
    owner_row = owner[...].astype(F32)
    ends = jnp.sum(
        jnp.where(iota((NSLICE, NSLICE), 1) <= iota((NSLICE, NSLICE), 0), width_row, 0.0),
        axis=1, keepdims=True,
    )
    first = b * BANDS
    band_row = (first + iota((1, BANDS), 1)).astype(F32)
    slice_row = jnp.sum(jnp.where(ends <= band_row, 1.0, 0.0), axis=0, keepdims=True)
    first_row = jnp.zeros((1, BANDS), F32) + first.astype(F32)
    first_slice = jnp.sum(jnp.where(ends <= first_row, 1.0, 0.0), axis=0, keepdims=True)
    row = iota((2 * ROWS, BANDS), 0)
    local = row & (ROWS - 1)
    slot = (local * 43) >> 8
    pseudo = (row >> 5) * HALF + local - slot * HALF
    sign_f = sign[...].astype(F32)
    signs = jnp.zeros((2 * ROWS, BANDS), F32)
    for j in range(NPS):
        signs = jnp.where(pseudo == j, sign_f[j : j + 1, :], signs)
    member = (slice_row - first_slice == slot.astype(F32)) & (local < SLOTS * HALF)
    mixing = jnp.where(member, signs, 0.0).astype(BF16)
    mixing = jnp.concatenate([mixing, mixing], axis=1)

    def partial_sums(p):
        loads[p].wait()

        @pl.loop(0, CHIPS // 2)
        def _(pair):
            part = coeffs[p, :, pl.ds(pl.multiple_of(pair * 256, 256), 256)]
            high = part.astype(BF16)
            low = (part - high.astype(F32)).astype(BF16)
            sums = jnp.dot(
                mixing, jnp.concatenate([high, low], axis=0), preferred_element_type=F32
            )
            for side in range(2):
                for half in range(2):
                    a_send[p, pair * 2 + side, half] = sums[
                        half * ROWS : (half + 1) * ROWS, side * 128 : (side + 1) * 128
                    ]

    def a_copy(p, dx, dy, dc):
        chip = chip_at(dx, dy)
        core = lax.rem(c + dc, 2)
        return pltpu.make_async_remote_copy(
            src_ref=a_send.at[p, chip, core],
            dst_ref=a_recv.at[p, b],
            send_sem=a_ssem.at[p],
            recv_sem=a_rsem.at[p],
            device_id=(chip * 2 + core, g),
            device_id_type=MESH,
        )

    def send_a(p):
        for dx, dy in OFFSETS:
            for dc in range(2):
                a_copy(p, dx, dy, dc).start()
        a_copy(p, 0, 0, 1).start()
        a_recv[p, b] = a_send[p, q, c]

    def a_all(p):
        return pltpu.make_async_remote_copy(
            src_ref=a_recv.at[p, pl.ds(0, GROUPS - 1)],
            dst_ref=a_recv.at[p, pl.ds(0, GROUPS - 1)],
            send_sem=a_ssem.at[p],
            recv_sem=a_rsem.at[p],
            device_id=(b, g),
            device_id_type=MESH,
        )

    partial_sums(0)
    pl.semaphore_wait(barrier, greeted)
    send_a(0)
    for p in range(1, PHASES):
        partial_sums(p)
        send_a(p)

    source = iota((1, GROUPS * ROWS), 1)
    source_local = source & (ROWS - 1)
    source_slot = (source_local * 43) >> 8
    source_half = jnp.where(
        source_local < SLOTS * HALF, source_local - source_slot * HALF, -1
    )
    source_first = ((source >> 5) * BANDS).astype(F32)
    source_slice = (
        jnp.sum(jnp.where(ends <= source_first, 1.0, 0.0), axis=0, keepdims=True)
        + source_slot.astype(F32)
    )
    block = OUT // 8
    for e in range(8):
        in_slot, h, cc = e >> 2, (e >> 1) & 1, e & 1
        r = iota((block, NSLICE), 0)
        chip = (r * 43) >> 7
        t = r - chip * 3
        place = (chip * 2 + cc) * 2 + in_slot
        lane = iota((block, NSLICE), 1)
        target = jnp.sum(jnp.where(lane == place, owner_row, 0.0), axis=1, keepdims=True)
        bands = jnp.sum(
            jnp.where(lane.astype(F32) == target, width_row, 0.0), axis=1, keepdims=True
        )
        scale[e * block : (e + 1) * block, :] = jnp.broadcast_to(1.0 / jnp.sqrt(bands), (block, 128))
        r2 = iota((block, GROUPS * ROWS), 0)
        t2 = r2 - ((r2 * 43) >> 7) * 3
        hit = (target == source_slice) & (t2 + 3 * h == source_half)
        select[e * block : (e + 1) * block, :] = jnp.where(hit, 1.0, 0.0).astype(BF16)

    in_class = lax.rem(g, 4) // 2 == c

    def combine(p):
        a_all(p).wait_recv()
        part = a_recv[p].reshape(GROUPS * ROWS, 128)
        high = part.astype(BF16)
        low = (part - high.astype(F32)).astype(BF16)
        both = jnp.dot(
            select[...], jnp.concatenate([high, low], axis=1), preferred_element_type=F32
        )
        rows = (both[:, :128] + both[:, 128:]) * scale[...]
        for e in range(8):
            z_send[p, e] = rows[e * block : (e + 1) * block].reshape(CHIPS, 3, 1, 128)

    def z_copy(p, e):
        plane = (e >> 2) * 4 + 2 * c + ((e >> 1) & 1)
        core = e & 1
        copy = pltpu.make_async_remote_copy(
            src_ref=z_send.at[p, e],
            dst_ref=z_recv.at[p, :, g],
            send_sem=z_ssem.at[p, e],
            recv_sem=z_rsem.at[p, g],
            device_id=(q * 2 + core, plane),
            device_id_type=MESH,
        )
        here = (plane == g) & (core == c)
        return copy, here

    def send_z(p):
        for e in range(8):
            copy, here = z_copy(p, e)

            @pl.when(jnp.logical_not(here))
            def _():
                copy.start()

            @pl.when(here)
            def _():
                z_recv[p, :, g] = z_send[p, e]

    def wait_z(p):
        for plane in range(NZ):
            copy = pltpu.make_async_remote_copy(
                src_ref=z_send.at[p, 0],
                dst_ref=z_recv.at[p, :, plane],
                send_sem=z_ssem.at[p, 0],
                recv_sem=z_rsem.at[p, plane],
                device_id=(b, g),
                device_id_type=MESH,
            )

            @pl.when(jnp.logical_not(in_class & (g == plane)))
            def _():
                copy.wait_recv()

    def b_copy(p, dx, dy):
        chip = chip_at(dx, dy)
        return pltpu.make_async_remote_copy(
            src_ref=z_recv.at[p, chip],
            dst_ref=out_ref.at[:, p, q],
            send_sem=b_ssem.at[p],
            recv_sem=b_rsem.at[p],
            device_id=(chip * 2 + c, g),
            device_id_type=MESH,
        )

    def send_b(p):
        for dx, dy in OFFSETS:
            b_copy(p, dx, dy).start()
        out_ref[:, p, q] = z_recv[p, q]

    def b_all(p):
        return pltpu.make_async_remote_copy(
            src_ref=z_recv.at[p, pl.ds(0, CHIPS - 1)],
            dst_ref=z_recv.at[p, pl.ds(0, CHIPS - 1)],
            send_sem=b_ssem.at[p],
            recv_sem=b_rsem.at[p],
            device_id=(b, g),
            device_id_type=MESH,
        )

    for p in range(PHASES):
        combine(p)
        send_z(p)
        if p > 0:
            wait_z(p - 1)
            send_b(p - 1)
    wait_z(PHASES - 1)
    send_b(PHASES - 1)

    for p in range(PHASES):
        b_all(p).wait_recv()
    for p in range(PHASES):
        a_all(p).wait_send()
        for e in range(8):
            copy, here = z_copy(p, e)

            @pl.when(jnp.logical_not(here))
            def _():
                copy.wait_send()

        b_all(p).wait_send()


def on_device(band_coeffs, sign_table, slice_widths, owner_map):
    hbm = pl.BlockSpec(memory_space=pl.ANY)
    rows = pl.pallas_call(
        kernel,
        out_shape=jax.ShapeDtypeStruct((NZ, PHASES, CHIPS, 3, 1, 128), F32),
        in_specs=[hbm] * 4,
        out_specs=pl.BlockSpec(memory_space=pltpu.VMEM),
        scratch_shapes=[
            pltpu.VMEM((PHASES, BANDS, WIDE), F32),
            pltpu.VMEM((NPS, BANDS), jnp.int32),
            pltpu.VMEM((1, NSLICE), jnp.int32),
            pltpu.VMEM((1, NSLICE), jnp.int32),
            pltpu.VMEM((OUT, GROUPS * ROWS), BF16),
            pltpu.VMEM((OUT, 128), F32),
            pltpu.VMEM((PHASES, CHIPS, 2, ROWS, 128), F32),
            pltpu.VMEM((PHASES, GROUPS, ROWS, 128), F32),
            pltpu.VMEM((PHASES, 8, CHIPS, 3, 1, 128), F32),
            pltpu.VMEM((PHASES, CHIPS, NZ, 3, 1, 128), F32),
            pltpu.SemaphoreType.DMA((PHASES,)),
            pltpu.SemaphoreType.DMA((3,)),
            pltpu.SemaphoreType.DMA((PHASES,)),
            pltpu.SemaphoreType.DMA((PHASES,)),
            pltpu.SemaphoreType.DMA((PHASES, 8)),
            pltpu.SemaphoreType.DMA((PHASES, NZ)),
            pltpu.SemaphoreType.DMA((PHASES,)),
            pltpu.SemaphoreType.DMA((PHASES,)),
        ],
        compiler_params=pltpu.CompilerParams(
            collective_id=0, has_side_effects=True, vmem_limit_bytes=60 * 2**20
        ),
        name="pseudobands",
    )(band_coeffs, sign_table, slice_widths.reshape(1, NSLICE), owner_map.reshape(1, NSLICE))
    return jnp.transpose(rows[:, :, :, :, 0, :], (3, 0, 1, 2, 4)).reshape(3, NZ * SLAB)


def solution(mesh):
    return jax.shard_map(
        on_device,
        mesh=mesh,
        in_specs=(P("band", "gslab"), P(None, "band"), P(), P()),
        out_specs=P(("band", "gslab"), None),
        check_vma=False,
    )
```

```python
import jax
import jax.numpy as jnp
from jax import lax
from jax.experimental import pallas as pl
from jax.experimental.pallas import tpu as pltpu
from jax.sharding import PartitionSpec as P

MESH = pl.DeviceIdType.MESH
F32 = jnp.float32
BF16 = jnp.bfloat16

NX, NY, NZ = 4, 4, 8
CHIPS = NX * NY
GROUPS = 2 * CHIPS
BANDS = 384
SLAB = 6144
PHASES = 3
WIDE = SLAB // PHASES
NPS = 12
TRI = 3
SLOTS = 5
ROWS = 16
NSLICE = 64
OUT = NSLICE * TRI
LAG = 2
VMEM_LIMIT = 52 * 10**6

OFFSETS = (
    (1, 0), (0, 1), (3, 0), (0, 3), (1, 1), (3, 3), (1, 3), (3, 1),
    (2, 0), (0, 2), (2, 1), (1, 2), (2, 3), (3, 2), (2, 2),
)


def iota(shape, dim):
    return lax.broadcasted_iota(jnp.int32, shape, dim)


def kernel(
    band_ref, sign_ref, width_ref, owner_ref, out_ref,
    coeffs, sign, width, owner, select, scale,
    a_send, a_recv, z_send, z_recv,
    load_sem, small_sem, a_ssem, a_rsem, z_ssem, z_rsem, b_ssem, b_rsem,
):
    b = lax.axis_index("band")
    g = lax.axis_index("gslab")
    c = lax.rem(b, 2)
    q = b // 2
    x = lax.rem(q, NX)
    y = q // NX
    parity = lax.rem(x + y, 2)

    def chip_at(dx, dy):
        return lax.rem(y + dy, NY) * NX + lax.rem(x + dx, NX)

    loads = [
        pltpu.make_async_copy(band_ref.at[:, pl.ds(p * WIDE, WIDE)], coeffs.at[p], load_sem.at[p])
        for p in range(PHASES)
    ]
    smalls = [
        pltpu.make_async_copy(src, dst, small_sem.at[i])
        for i, (src, dst) in enumerate(((sign_ref, sign), (width_ref, width), (owner_ref, owner)))
    ]
    for copy in smalls:
        copy.start()
    loads[0].start()

    barrier = pltpu.get_barrier_semaphore()
    greeted = 0
    for dc in range(2):
        for dx, dy in ((0, 0),) + OFFSETS:
            if (dc, dx, dy) != (0, 0, 0):
                peer = chip_at(dx, dy) * 2 + lax.rem(c + dc, 2)
                pl.semaphore_signal(barrier, inc=1, device_id=(peer, g), device_id_type=MESH)
                greeted += 1
        for dz in range(1, NZ):
            peer = q * 2 + lax.rem(c + dc, 2)
            pl.semaphore_signal(
                barrier, inc=1, device_id=(peer, lax.rem(g + dz, NZ)), device_id_type=MESH
            )
            greeted += 1
    for copy in loads[1:]:
        copy.start()

    for copy in smalls:
        copy.wait()
    width_row = width[...].astype(F32)
    owner_row = owner[...].astype(F32)
    ends = jnp.sum(
        jnp.where(iota((NSLICE, NSLICE), 1) <= iota((NSLICE, NSLICE), 0), width_row, 0.0),
        axis=1, keepdims=True,
    )
    first = b * BANDS
    band_row = (first + iota((1, BANDS), 1)).astype(F32)
    slice_row = jnp.sum(jnp.where(ends <= band_row, 1.0, 0.0), axis=0, keepdims=True)
    first_row = jnp.zeros((1, BANDS), F32) + first.astype(F32)
    first_slice = jnp.sum(jnp.where(ends <= first_row, 1.0, 0.0), axis=0, keepdims=True)
    row = iota((4 * ROWS, BANDS), 0)
    local = row & (ROWS - 1)
    slot = (local * 11) >> 5
    pseudo = (row >> 4) * TRI + local - slot * TRI
    sign_f = sign[...].astype(F32)
    signs = jnp.zeros((4 * ROWS, BANDS), F32)
    for j in range(NPS):
        signs = jnp.where(pseudo == j, sign_f[j : j + 1, :], signs)
    member = (slice_row - first_slice == slot.astype(F32)) & (local < SLOTS * TRI)
    mixing = jnp.where(member, signs, 0.0).astype(BF16)
    mixing = jnp.concatenate([mixing, mixing], axis=1)

    def partial_sums(p):
        loads[p].wait()

        @pl.loop(0, CHIPS // 2)
        def _(pair):
            part = coeffs[p, :, pl.ds(pl.multiple_of(pair * 256, 256), 256)]
            high = part.astype(BF16)
            low = (part - high.astype(F32)).astype(BF16)
            sums = jnp.dot(
                mixing, jnp.concatenate([high, low], axis=0), preferred_element_type=F32
            )
            for side in range(2):
                for part in range(4):
                    a_send[p, pair * 2 + side, part] = sums[
                        part * ROWS : (part + 1) * ROWS, side * 128 : (side + 1) * 128
                    ]

    def a_copy(p, s, dx, dy, dc):
        chip = chip_at(dx, dy)
        core = lax.rem(c + dc, 2)
        return pltpu.make_async_remote_copy(
            src_ref=a_send.at[p, chip, core * 2 + lax.rem(parity + (s + dx + dy), 2)],
            dst_ref=a_recv.at[p, s, b],
            send_sem=a_ssem.at[p, s],
            recv_sem=a_rsem.at[p, s],
            device_id=(chip * 2 + core, g),
            device_id_type=MESH,
        )

    def send_a(p):
        for s in range(2):
            for dx, dy in OFFSETS:
                for dc in range(2):
                    a_copy(p, s, dx, dy, dc).start()
            a_copy(p, s, 0, 0, 1).start()
            a_recv[p, s, b] = a_send[p, q, c * 2 + lax.rem(parity + s, 2)]

    def a_all(p, s):
        return pltpu.make_async_remote_copy(
            src_ref=a_recv.at[p, s, pl.ds(0, GROUPS - 1)],
            dst_ref=a_recv.at[p, s, pl.ds(0, GROUPS - 1)],
            send_sem=a_ssem.at[p, s],
            recv_sem=a_rsem.at[p, s],
            device_id=(b, g),
            device_id_type=MESH,
        )

    with jax.named_scope("sums#p=0"):
        partial_sums(0)
    with jax.named_scope("barrier"):
        pl.semaphore_wait(barrier, greeted)
    with jax.named_scope("send_a#p=0"):
        send_a(0)
    for p in range(1, PHASES):
        with jax.named_scope(f"sums#p={p}"):
            partial_sums(p)
        with jax.named_scope(f"send_a#p={p}"):
            send_a(p)

    source = iota((1, GROUPS * ROWS), 1)
    source_local = source & (ROWS - 1)
    source_slot = (source_local * 11) >> 5
    source_t = jnp.where(source_local < SLOTS * TRI, source_local - source_slot * TRI, -1)
    source_first = ((source >> 4) * BANDS).astype(F32)
    source_slice = (
        jnp.sum(jnp.where(ends <= source_first, 1.0, 0.0), axis=0, keepdims=True)
        + source_slot.astype(F32)
    )
    block = OUT // 4
    for e in range(4):
        in_slot, cc = e >> 1, e & 1
        r = iota((block, NSLICE), 0)
        place = (((r * 43) >> 7) * 2 + cc) * 2 + in_slot
        lane = iota((block, NSLICE), 1)
        target = jnp.sum(jnp.where(lane == place, owner_row, 0.0), axis=1, keepdims=True)
        bands = jnp.sum(
            jnp.where(lane.astype(F32) == target, width_row, 0.0), axis=1, keepdims=True
        )
        scale[e * block : (e + 1) * block, :] = jnp.broadcast_to(1.0 / jnp.sqrt(bands), (block, 128))
        r2 = iota((block, GROUPS * ROWS), 0)
        t2 = r2 - ((r2 * 43) >> 7) * TRI
        hit = (target == source_slice) & (t2 == source_t)
        select[e * block : (e + 1) * block, :] = jnp.where(hit, 1.0, 0.0).astype(BF16)

    in_class = lax.rem(g, 4) // 2 == c

    def combine(p, s):
        with jax.named_scope(f"wait_a#p={p}#s={s}"):
            a_all(p, s).wait_recv()
        part = a_recv[p, s].reshape(GROUPS * ROWS, 128)
        high = part.astype(BF16)
        low = (part - high.astype(F32)).astype(BF16)
        both = jnp.dot(
            select[...], jnp.concatenate([high, low], axis=1), preferred_element_type=F32
        )
        rows = (both[:, :128] + both[:, 128:]) * scale[...]
        for e in range(4):
            z_send[p, s, e] = rows[e * block : (e + 1) * block].reshape(CHIPS, TRI, 128)

    def z_copy(p, s, e):
        plane = (e >> 1) * 4 + 2 * c + lax.rem(parity + s, 2)
        core = e & 1
        copy = pltpu.make_async_remote_copy(
            src_ref=z_send.at[p, s, e],
            dst_ref=z_recv.at[p, :, g],
            send_sem=z_ssem.at[p, s, e],
            recv_sem=z_rsem.at[p, g],
            device_id=(q * 2 + core, plane),
            device_id_type=MESH,
        )
        here = (plane == g) & (core == c)
        return copy, here

    def send_z(p, s):
        for e in range(4):
            copy, here = z_copy(p, s, e)

            @pl.when(jnp.logical_not(here))
            def _():
                copy.start()

            @pl.when(here)
            def _():
                z_recv[p, :, g] = z_send[p, s, e]

    def wait_z(p):
        for plane in range(NZ):
            copy = pltpu.make_async_remote_copy(
                src_ref=z_send.at[p, 0, 0],
                dst_ref=z_recv.at[p, :, plane],
                send_sem=z_ssem.at[p, 0, 0],
                recv_sem=z_rsem.at[p, plane],
                device_id=(b, g),
                device_id_type=MESH,
            )

            @pl.when(jnp.logical_not(in_class & (g == plane)))
            def _():
                copy.wait_recv()

    def b_copy(p, dx, dy):
        chip = chip_at(dx, dy)
        return pltpu.make_async_remote_copy(
            src_ref=z_recv.at[p, chip],
            dst_ref=out_ref.at[:, p, q],
            send_sem=b_ssem.at[p],
            recv_sem=b_rsem.at[p],
            device_id=(chip * 2 + c, g),
            device_id_type=MESH,
        )

    def b_all(p):
        return pltpu.make_async_remote_copy(
            src_ref=z_recv.at[p, pl.ds(0, CHIPS - 1)],
            dst_ref=z_recv.at[p, pl.ds(0, CHIPS - 1)],
            send_sem=b_ssem.at[p],
            recv_sem=b_rsem.at[p],
            device_id=(b, g),
            device_id_type=MESH,
        )

    mine = lax.rem(g + parity, 2)

    def pass_on(p, s):
        @pl.when(mine == s)
        def _():
            with jax.named_scope(f"wait_z#p={p}#s={s}"):
                wait_z(p)
            for dx, dy in OFFSETS:
                b_copy(p, dx, dy).start()
            out_ref[:, p, q] = z_recv[p, q]

    steps = [(p, s) for p in range(PHASES) for s in range(2)]
    for k, step in enumerate(steps):
        combine(*step)
        with jax.named_scope(f"send_z#p={step[0]}#s={step[1]}"):
            send_z(*step)
        if k >= LAG:
            pass_on(*steps[k - LAG])
    for step in steps[-LAG:]:
        pass_on(*step)

    for p in range(PHASES):
        with jax.named_scope(f"wait_b#p={p}"):
            b_all(p).wait_recv()
    for p in range(PHASES):
        for s in range(2):
            a_all(p, s).wait_send()
            for e in range(4):
                copy, here = z_copy(p, s, e)

                @pl.when(jnp.logical_not(here))
                def _():
                    copy.wait_send()

        b_all(p).wait_send()


def on_device(band_coeffs, sign_table, slice_widths, owner_map):
    hbm = pl.BlockSpec(memory_space=pltpu.HBM)
    operands = (band_coeffs, sign_table, slice_widths.reshape(1, NSLICE), owner_map.reshape(1, NSLICE))
    operands = [pltpu.with_memory_space_constraint(v, pltpu.HBM) for v in operands]
    rows = pl.pallas_call(
        kernel,
        out_shape=jax.ShapeDtypeStruct((NZ, PHASES, CHIPS, TRI, 128), F32),
        in_specs=[hbm] * 4,
        out_specs=pl.BlockSpec(memory_space=pltpu.VMEM),
        scratch_shapes=[
            pltpu.VMEM((PHASES, BANDS, WIDE), F32),
            pltpu.VMEM((NPS, BANDS), jnp.int32),
            pltpu.VMEM((1, NSLICE), jnp.int32),
            pltpu.VMEM((1, NSLICE), jnp.int32),
            pltpu.VMEM((OUT, GROUPS * ROWS), BF16),
            pltpu.VMEM((OUT, 128), F32),
            pltpu.VMEM((PHASES, CHIPS, 4, ROWS, 128), F32),
            pltpu.VMEM((PHASES, 2, GROUPS, ROWS, 128), F32),
            pltpu.VMEM((PHASES, 2, 4, CHIPS, TRI, 128), F32),
            pltpu.VMEM((PHASES, CHIPS, NZ, TRI, 128), F32),
            pltpu.SemaphoreType.DMA((PHASES,)),
            pltpu.SemaphoreType.DMA((3,)),
            pltpu.SemaphoreType.DMA((PHASES, 2)),
            pltpu.SemaphoreType.DMA((PHASES, 2)),
            pltpu.SemaphoreType.DMA((PHASES, 2, 4)),
            pltpu.SemaphoreType.DMA((PHASES, NZ)),
            pltpu.SemaphoreType.DMA((PHASES,)),
            pltpu.SemaphoreType.DMA((PHASES,)),
        ],
        compiler_params=pltpu.CompilerParams(
            collective_id=0, has_side_effects=True, vmem_limit_bytes=VMEM_LIMIT
        ),
        name="pseudobands",
    )(*operands)
    return jnp.transpose(rows.reshape(-1, TRI, 128), (1, 0, 2)).reshape(TRI, NZ * SLAB)


def solution(mesh):
    return jax.shard_map(
        on_device,
        mesh=mesh,
        in_specs=(P("band", "gslab"), P(None, "band"), P(), P()),
        out_specs=P(("band", "gslab"), None),
        check_vma=False,
    )
```

```python
import jax
import jax.numpy as jnp
from jax import lax
from jax.experimental import pallas as pl
from jax.experimental.pallas import tpu as pltpu
from jax.sharding import PartitionSpec as P

MESH = pl.DeviceIdType.MESH
F32 = jnp.float32
BF16 = jnp.bfloat16

NX, NY, NZ = 4, 4, 8
CHIPS = NX * NY
GROUPS = 2 * CHIPS
BANDS = 384
SLAB = 6144
PHASES = 3
WIDE = SLAB // PHASES
NPS = 12
TRI = 3
SLOTS = 5
ROWS = 16
USED = SLOTS * TRI
NSLICE = 64
OUT = NSLICE * TRI
LAG = 2
DIRECT = ((2, 0), (2, 1))
VMEM_LIMIT = 52 * 10**6

OFFSETS = (
    (1, 0), (0, 1), (3, 0), (0, 3), (1, 1), (3, 3), (1, 3), (3, 1),
    (2, 0), (0, 2), (2, 1), (1, 2), (2, 3), (3, 2), (2, 2),
)

A_ORDER = ((2, 2), (2, 1), (2, 3), (2, 0), (1, 2), (3, 2), (1, 1), (3, 3), (1, 3), (3, 1), (1, 0), (3, 0), (0, 2), (0, 1), (0, 3))


def iota(shape, dim):
    return lax.broadcasted_iota(jnp.int32, shape, dim)


def kernel(
    band_ref, sign_ref, width_ref, owner_ref, out_ref,
    coeffs, sign, width, owner, select, scale,
    a_send, a_recv, z_send, z_recv,
    load_sem, small_sem, a_ssem, a_rsem, z_ssem, z_rsem, b_ssem, b_rsem,
):
    b = lax.axis_index("band")
    g = lax.axis_index("gslab")
    c = lax.rem(b, 2)
    q = b // 2
    x = lax.rem(q, NX)
    y = q // NX
    parity = lax.rem(x + y, 2)

    def chip_at(dx, dy):
        return lax.rem(y + dy, NY) * NX + lax.rem(x + dx, NX)

    loads = [
        pltpu.make_async_copy(band_ref.at[:, pl.ds(p * WIDE, WIDE)], coeffs.at[p], load_sem.at[p])
        for p in range(PHASES)
    ]
    smalls = [
        pltpu.make_async_copy(src, dst, small_sem.at[i])
        for i, (src, dst) in enumerate(((sign_ref, sign), (width_ref, width), (owner_ref, owner)))
    ]
    for copy in smalls:
        copy.start()
    loads[0].start()

    barrier = pltpu.get_barrier_semaphore()
    greeted = 0
    for dz in (4, 3, 5, 2, 6, 1, 7):
        for core in range(2):
            pl.semaphore_signal(
                barrier, inc=1, device_id=(q * 2 + core, lax.rem(g + dz, NZ)), device_id_type=MESH
            )
            greeted += 1
    for dx, dy in reversed(OFFSETS):
        for core in range(2):
            pl.semaphore_signal(
                barrier, inc=1, device_id=(chip_at(dx, dy) * 2 + core, g), device_id_type=MESH
            )
            greeted += 1
    pl.semaphore_signal(barrier, inc=1, device_id=(q * 2 + 1 - c, g), device_id_type=MESH)
    greeted += 1
    for copy in loads[1:]:
        copy.start()

    for copy in smalls:
        copy.wait()
    width_row = width[...].astype(F32)
    owner_row = owner[...].astype(F32)
    ends = jnp.sum(
        jnp.where(iota((NSLICE, NSLICE), 1) <= iota((NSLICE, NSLICE), 0), width_row, 0.0),
        axis=1, keepdims=True,
    )
    first = b * BANDS
    band_row = (first + iota((1, BANDS), 1)).astype(F32)
    slice_row = jnp.sum(jnp.where(ends <= band_row, 1.0, 0.0), axis=0, keepdims=True)
    first_row = jnp.zeros((1, BANDS), F32) + first.astype(F32)
    first_slice = jnp.sum(jnp.where(ends <= first_row, 1.0, 0.0), axis=0, keepdims=True)
    row = iota((4 * ROWS, BANDS), 0)
    local = row & (ROWS - 1)
    slot = (local * 11) >> 5
    pseudo = (row >> 4) * TRI + local - slot * TRI
    sign_f = sign[...].astype(F32)
    signs = jnp.zeros((4 * ROWS, BANDS), F32)
    for j in range(NPS):
        signs = jnp.where(pseudo == j, sign_f[j : j + 1, :], signs)
    member = (slice_row - first_slice == slot.astype(F32)) & (local < SLOTS * TRI)
    mixing = jnp.where(member, signs, 0.0).astype(BF16)
    mixing = jnp.concatenate([mixing, mixing], axis=1)

    def partial_sums(p):
        loads[p].wait()

        @pl.loop(0, CHIPS // 2)
        def _(pair):
            part = coeffs[p, :, pl.ds(pl.multiple_of(pair * 256, 256), 256)]
            high = part.astype(BF16)
            low = (part - high.astype(F32)).astype(BF16)
            sums = jnp.dot(
                mixing, jnp.concatenate([high, low], axis=0), preferred_element_type=F32
            )
            for side in range(2):
                for part in range(4):
                    a_send[p, pair * 2 + side, part] = sums[
                        part * ROWS : part * ROWS + USED, side * 128 : (side + 1) * 128
                    ]

    def a_copy(p, s, dx, dy, dc):
        chip = chip_at(dx, dy)
        core = lax.rem(c + dc, 2)
        return pltpu.make_async_remote_copy(
            src_ref=a_send.at[p, chip, core * 2 + lax.rem(parity + (s + dx + dy), 2)],
            dst_ref=a_recv.at[p, s, b],
            send_sem=a_ssem.at[p, s],
            recv_sem=a_rsem.at[p, s],
            device_id=(chip * 2 + core, g),
            device_id_type=MESH,
        )

    def send_a(p):
        for s in range(2):
            for dx, dy in A_ORDER:
                for dc in range(2):
                    a_copy(p, s, dx, dy, dc).start()
            a_copy(p, s, 0, 0, 1).start()
            a_recv[p, s, b] = a_send[p, q, c * 2 + lax.rem(parity + s, 2)]

    def a_all(p, s):
        return pltpu.make_async_remote_copy(
            src_ref=a_recv.at[p, s, pl.ds(0, GROUPS - 1)],
            dst_ref=a_recv.at[p, s, pl.ds(0, GROUPS - 1)],
            send_sem=a_ssem.at[p, s],
            recv_sem=a_rsem.at[p, s],
            device_id=(b, g),
            device_id_type=MESH,
        )

    with jax.named_scope("sums#p=0"):
        partial_sums(0)
    with jax.named_scope("barrier"):
        pl.semaphore_wait(barrier, greeted)
    with jax.named_scope("send_a#p=0"):
        send_a(0)
    for p in range(1, PHASES):
        with jax.named_scope(f"sums#p={p}"):
            partial_sums(p)
        with jax.named_scope(f"send_a#p={p}"):
            send_a(p)

    source = iota((1, GROUPS * ROWS), 1)
    source_local = source & (ROWS - 1)
    source_slot = (source_local * 11) >> 5
    source_t = jnp.where(source_local < SLOTS * TRI, source_local - source_slot * TRI, -1)
    source_first = ((source >> 4) * BANDS).astype(F32)
    source_slice = (
        jnp.sum(jnp.where(ends <= source_first, 1.0, 0.0), axis=0, keepdims=True)
        + source_slot.astype(F32)
    )
    block = OUT // 4
    for e in range(4):
        in_slot, cc = e >> 1, e & 1
        r = iota((block, NSLICE), 0)
        place = (((r * 43) >> 7) * 2 + cc) * 2 + in_slot
        lane = iota((block, NSLICE), 1)
        target = jnp.sum(jnp.where(lane == place, owner_row, 0.0), axis=1, keepdims=True)
        bands = jnp.sum(
            jnp.where(lane.astype(F32) == target, width_row, 0.0), axis=1, keepdims=True
        )
        scale[e * block : (e + 1) * block, :] = jnp.broadcast_to(1.0 / jnp.sqrt(bands), (block, 128))
        r2 = iota((block, GROUPS * ROWS), 0)
        t2 = r2 - ((r2 * 43) >> 7) * TRI
        hit = (target == source_slice) & (t2 == source_t)
        select[e * block : (e + 1) * block, :] = jnp.where(hit, 1.0, 0.0).astype(BF16)

    in_class = lax.rem(g, 4) // 2 == c

    def z_rows(s, e):
        return pl.ds((s * 4 + e) * CHIPS, CHIPS)

    def combine(p, s):
        with jax.named_scope(f"wait_a#p={p}#s={s}"):
            a_all(p, s).wait_recv()
        part = jnp.concatenate([a_recv[p, s], jnp.zeros((GROUPS, ROWS - USED, 128), F32)], axis=1)
        part = part.reshape(GROUPS * ROWS, 128)
        high = part.astype(BF16)
        low = (part - high.astype(F32)).astype(BF16)
        both = jnp.dot(
            select[...], jnp.concatenate([high, low], axis=1), preferred_element_type=F32
        )
        rows = (both[:, :128] + both[:, 128:]) * scale[...]
        for e in range(4):
            z_send[p, z_rows(s, e)] = rows[e * block : (e + 1) * block].reshape(CHIPS, TRI, 128)

    def z_copy(p, s, e):
        plane = (e >> 1) * 4 + 2 * c + lax.rem(parity + s, 2)
        core = e & 1
        copy = pltpu.make_async_remote_copy(
            src_ref=z_send.at[p, z_rows(s, e)],
            dst_ref=z_recv.at[p, :, g],
            send_sem=z_ssem.at[p, s, e],
            recv_sem=z_rsem.at[p, g],
            device_id=(q * 2 + core, plane),
            device_id_type=MESH,
        )
        here = (plane == g) & (core == c)
        return copy, here

    def send_z(p, s):
        for e in range(4):
            copy, here = z_copy(p, s, e)

            @pl.when(jnp.logical_not(here))
            def _():
                copy.start()

            @pl.when(here)
            def _():
                z_recv[p, :, g] = z_send[p, z_rows(s, e)]

    def wait_z(p):
        for plane in range(NZ):
            copy = pltpu.make_async_remote_copy(
                src_ref=z_send.at[p, z_rows(0, 0)],
                dst_ref=z_recv.at[p, :, plane],
                send_sem=z_ssem.at[p, 0, 0],
                recv_sem=z_rsem.at[p, plane],
                device_id=(b, g),
                device_id_type=MESH,
            )

            @pl.when(jnp.logical_not(in_class & (g == plane)))
            def _():
                copy.wait_recv()

    def b_copy(p, dx, dy):
        chip = chip_at(dx, dy)
        return pltpu.make_async_remote_copy(
            src_ref=z_recv.at[p, chip],
            dst_ref=out_ref.at[:, p, q],
            send_sem=b_ssem.at[p],
            recv_sem=b_rsem.at[p],
            device_id=(chip * 2 + c, g),
            device_id_type=MESH,
        )

    def b_all(p):
        return pltpu.make_async_remote_copy(
            src_ref=z_recv.at[p, pl.ds(0, CHIPS - 1)],
            dst_ref=z_recv.at[p, pl.ds(0, CHIPS - 1)],
            send_sem=b_ssem.at[p],
            recv_sem=b_rsem.at[p],
            device_id=(b, g),
            device_id_type=MESH,
        )

    def d_copy(p, s, e, dx, dy):
        plane = (e >> 1) * 4 + 2 * c + lax.rem(parity + s, 2)
        core = e & 1
        chip = chip_at(dx, dy)
        copy = pltpu.make_async_remote_copy(
            src_ref=z_send.at[p, (s * 4 + e) * CHIPS + chip],
            dst_ref=out_ref.at[g, p, q],
            send_sem=z_ssem.at[p, s, 0],
            recv_sem=b_rsem.at[p],
            device_id=(chip * 2 + core, plane),
            device_id_type=MESH,
        )
        return copy, (plane == g) & (core == c)

    def send_d(p, s):
        for dx, dy in tuple(reversed(OFFSETS)):
            for e in range(4):
                d_copy(p, s, e, dx, dy)[0].start()
        for e in range(4):
            copy, here = d_copy(p, s, e, 0, 0)

            @pl.when(jnp.logical_not(here))
            def _():
                copy.start()

            @pl.when(here)
            def _():
                out_ref[g, p, q] = z_send[p, (s * 4 + e) * CHIPS + q]

    def d_all(p, s, count):
        return pltpu.make_async_remote_copy(
            src_ref=z_send.at[p, pl.ds(0, count)],
            dst_ref=z_send.at[p, pl.ds(0, count)],
            send_sem=z_ssem.at[p, s, 0],
            recv_sem=b_rsem.at[p],
            device_id=(b, g),
            device_id_type=MESH,
        )

    mine = lax.rem(g + parity, 2)

    def pass_on(p, s):
        @pl.when(mine == s)
        def _():
            with jax.named_scope(f"wait_z#p={p}#s={s}"):
                wait_z(p)
            for dx, dy in reversed(OFFSETS):
                b_copy(p, dx, dy).start()
            out_ref[:, p, q] = z_recv[p, q]

    steps = [(p, s) for p in range(PHASES) for s in range(2)]
    for k, step in enumerate(steps):
        combine(*step)
        with jax.named_scope(f"send_z#p={step[0]}#s={step[1]}"):
            (send_d if step in DIRECT else send_z)(*step)
        if k >= LAG and steps[k - LAG] not in DIRECT:
            pass_on(*steps[k - LAG])
    for step in steps[-LAG:]:
        if step not in DIRECT:
            pass_on(*step)

    for p in range(PHASES):
        for s in range(2):
            a_all(p, s).wait_send()
            if (p, s) in DIRECT:
                own = in_class & (mine == s)

                @pl.when(own)
                def _():
                    d_all(p, s, 4 * CHIPS - 1).wait_send()

                @pl.when(jnp.logical_not(own))
                def _():
                    d_all(p, s, 4 * CHIPS).wait_send()

            else:
                for e in range(4):
                    copy, here = z_copy(p, s, e)

                    @pl.when(jnp.logical_not(here))
                    def _():
                        copy.wait_send()

    for p in range(PHASES):
        for s in range(2):

            @pl.when(mine == s)
            def _():
                with jax.named_scope(f"wait_b#p={p}#s={s}"):
                    if (p, s) in DIRECT:

                        @pl.when(in_class)
                        def _():
                            d_all(p, s, NZ * CHIPS - 1).wait_recv()

                        @pl.when(jnp.logical_not(in_class))
                        def _():
                            d_all(p, s, NZ * CHIPS).wait_recv()

                    else:
                        b_all(p).wait_recv()
                        b_all(p).wait_send()


def on_device(band_coeffs, sign_table, slice_widths, owner_map):
    hbm = pl.BlockSpec(memory_space=pltpu.HBM)
    operands = (band_coeffs, sign_table, slice_widths.reshape(1, NSLICE), owner_map.reshape(1, NSLICE))
    operands = [pltpu.with_memory_space_constraint(v, pltpu.HBM) for v in operands]
    rows = pl.pallas_call(
        kernel,
        out_shape=jax.ShapeDtypeStruct((NZ, PHASES, CHIPS, TRI, 128), F32),
        in_specs=[hbm] * 4,
        out_specs=pl.BlockSpec(memory_space=pltpu.VMEM),
        scratch_shapes=[
            pltpu.VMEM((PHASES, BANDS, WIDE), F32),
            pltpu.VMEM((NPS, BANDS), jnp.int32),
            pltpu.VMEM((1, NSLICE), jnp.int32),
            pltpu.VMEM((1, NSLICE), jnp.int32),
            pltpu.VMEM((OUT, GROUPS * ROWS), BF16),
            pltpu.VMEM((OUT, 128), F32),
            pltpu.VMEM((PHASES, CHIPS, 4, USED, 128), F32),
            pltpu.VMEM((PHASES, 2, GROUPS, USED, 128), F32),
            pltpu.VMEM((PHASES, 2 * 4 * CHIPS, TRI, 128), F32),
            pltpu.VMEM((PHASES, CHIPS, NZ, TRI, 128), F32),
            pltpu.SemaphoreType.DMA((PHASES,)),
            pltpu.SemaphoreType.DMA((3,)),
            pltpu.SemaphoreType.DMA((PHASES, 2)),
            pltpu.SemaphoreType.DMA((PHASES, 2)),
            pltpu.SemaphoreType.DMA((PHASES, 2, 4)),
            pltpu.SemaphoreType.DMA((PHASES, NZ)),
            pltpu.SemaphoreType.DMA((PHASES,)),
            pltpu.SemaphoreType.DMA((PHASES,)),
        ],
        compiler_params=pltpu.CompilerParams(
            collective_id=0, has_side_effects=True, vmem_limit_bytes=VMEM_LIMIT
        ),
        name="pseudobands",
    )(*operands)
    return jnp.transpose(rows.reshape(-1, TRI, 128), (1, 0, 2)).reshape(TRI, NZ * SLAB)


def solution(mesh):
    return jax.shard_map(
        on_device,
        mesh=mesh,
        in_specs=(P("band", "gslab"), P(None, "band"), P(), P()),
        out_specs=P(("band", "gslab"), None),
        check_vma=False,
    )
```

```python
import jax
import jax.numpy as jnp
from jax import lax
from jax.experimental import pallas as pl
from jax.experimental.pallas import tpu as pltpu
from jax.sharding import PartitionSpec as P

MESH = pl.DeviceIdType.MESH
F32 = jnp.float32
BF16 = jnp.bfloat16

NX, NY, NZ = 4, 4, 8
CHIPS = NX * NY
GROUPS = 2 * CHIPS
BANDS = 384
SLAB = 6144
PHASES = 3
WIDE = SLAB // PHASES
NPS = 12
TRI = 3
SLOTS = 5
ROWS = 16
USED = SLOTS * TRI
CHIP_SLOTS = 9
CHIP_ROWS = 32
CHIP_USED = CHIP_SLOTS * TRI
NSLICE = 64
OUT = NSLICE * TRI
LAG = 2
DIRECT = ((2, 0), (2, 1))
VMEM_LIMIT = 52 * 10**6

OFFSETS = (
    (1, 0), (0, 1), (3, 0), (0, 3), (1, 1), (3, 3), (1, 3), (3, 1),
    (2, 0), (0, 2), (2, 1), (1, 2), (2, 3), (3, 2), (2, 2),
)

A_ORDER = ((2, 2), (2, 1), (2, 3), (2, 0), (1, 2), (3, 2), (1, 1), (3, 3), (1, 3), (3, 1), (1, 0), (3, 0), (0, 2), (0, 1), (0, 3))


def iota(shape, dim):
    return lax.broadcasted_iota(jnp.int32, shape, dim)


def kernel(
    band_ref, sign_ref, width_ref, owner_ref, out_ref,
    coeffs, sign, width, owner, select, chip_select, scale,
    a_send, a_recv, d_send, d_recv, m_send, m_recv, z_send, z_recv,
    load_sem, small_sem, a_ssem, a_rsem, d_ssem, d_rsem, z_ssem, b_ssem, b_rsem,
):
    b = lax.axis_index("band")
    g = lax.axis_index("gslab")
    c = lax.rem(b, 2)
    q = b // 2
    x = lax.rem(q, NX)
    y = q // NX
    parity = lax.rem(x + y, 2)

    def chip_at(dx, dy):
        return lax.rem(y + dy, NY) * NX + lax.rem(x + dx, NX)

    loads = [
        pltpu.make_async_copy(band_ref.at[:, pl.ds(p * WIDE, WIDE)], coeffs.at[p], load_sem.at[p])
        for p in range(PHASES)
    ]
    smalls = [
        pltpu.make_async_copy(src, dst, small_sem.at[i])
        for i, (src, dst) in enumerate(((sign_ref, sign), (width_ref, width), (owner_ref, owner)))
    ]
    for copy in smalls:
        copy.start()
    loads[0].start()

    barrier = pltpu.get_barrier_semaphore()
    greeted = 0
    for dz in (4, 3, 5, 2, 6, 1, 7):
        for core in range(2):
            pl.semaphore_signal(
                barrier, inc=1, device_id=(q * 2 + core, lax.rem(g + dz, NZ)), device_id_type=MESH
            )
            greeted += 1
    for dx, dy in reversed(OFFSETS):
        for core in range(2):
            pl.semaphore_signal(
                barrier, inc=1, device_id=(chip_at(dx, dy) * 2 + core, g), device_id_type=MESH
            )
            greeted += 1
    pl.semaphore_signal(barrier, inc=1, device_id=(q * 2 + 1 - c, g), device_id_type=MESH)
    greeted += 1
    for copy in loads[1:]:
        copy.start()

    for copy in smalls:
        copy.wait()
    width_row = width[...].astype(F32)
    owner_row = owner[...].astype(F32)
    ends = jnp.sum(
        jnp.where(iota((NSLICE, NSLICE), 1) <= iota((NSLICE, NSLICE), 0), width_row, 0.0),
        axis=1, keepdims=True,
    )
    first = b * BANDS
    band_row = (first + iota((1, BANDS), 1)).astype(F32)
    slice_row = jnp.sum(jnp.where(ends <= band_row, 1.0, 0.0), axis=0, keepdims=True)
    first_row = jnp.zeros((1, BANDS), F32) + first.astype(F32)
    first_slice = jnp.sum(jnp.where(ends <= first_row, 1.0, 0.0), axis=0, keepdims=True)
    row = iota((4 * ROWS, BANDS), 0)
    local = row & (ROWS - 1)
    slot = (local * 11) >> 5
    pseudo = (row >> 4) * TRI + local - slot * TRI
    sign_f = sign[...].astype(F32)
    signs = jnp.zeros((4 * ROWS, BANDS), F32)
    for j in range(NPS):
        signs = jnp.where(pseudo == j, sign_f[j : j + 1, :], signs)
    member = (slice_row - first_slice == slot.astype(F32)) & (local < SLOTS * TRI)
    mixing = jnp.where(member, signs, 0.0).astype(BF16)
    mixing = jnp.concatenate([mixing, mixing], axis=1)

    def chip_mixing():
        row = iota((4 * CHIP_ROWS, BANDS), 0)
        local = row & (CHIP_ROWS - 1)
        slot = (local * 11) >> 5
        half = jnp.where(row < 2 * CHIP_ROWS, c, 1 - c)
        pseudo = (half * 2 + ((row >> 5) & 1)) * TRI + local - slot * TRI
        signs = jnp.zeros((4 * CHIP_ROWS, BANDS), F32)
        for j in range(NPS):
            signs = jnp.where(pseudo == j, sign_f[j : j + 1, :], signs)
        chip_row = jnp.zeros((1, BANDS), F32) + (q * (2 * BANDS)).astype(F32)
        chip_slice = jnp.sum(jnp.where(ends <= chip_row, 1.0, 0.0), axis=0, keepdims=True)
        member = (slice_row - chip_slice == slot.astype(F32)) & (local < CHIP_USED)
        mixing = jnp.where(member, signs, 0.0).astype(BF16)
        return jnp.concatenate([mixing, mixing], axis=1)

    def partial_sums(p, mixing, store):
        loads[p].wait()

        @pl.loop(0, CHIPS // 2, unroll=4)
        def _(pair):
            part = coeffs[p, :, pl.ds(pl.multiple_of(pair * 256, 256), 256)]
            high = part.astype(BF16)
            low = (part - high.astype(F32)).astype(BF16)
            sums = jnp.dot(
                mixing, jnp.concatenate([high, low], axis=0), preferred_element_type=F32
            )
            for side in range(2):
                store(pair * 2 + side, sums[:, side * 128 : (side + 1) * 128])

    def store_groups(chip, sums):
        for part in range(4):
            a_send[chip, part] = sums[part * ROWS : part * ROWS + USED]

    def store_chips(p):
        def store(chip, sums):
            for h in range(2):
                own = h * CHIP_ROWS
                m_send[p - 1, chip, h] = sums[own : own + CHIP_USED]
                other = own + 2 * CHIP_ROWS
                d_send[p - 1, chip, h] = sums[other : other + CHIP_USED]

        return store

    def a_copy(s, dx, dy, dc):
        chip = chip_at(dx, dy)
        core = lax.rem(c + dc, 2)
        return pltpu.make_async_remote_copy(
            src_ref=a_send.at[chip, core * 2 + lax.rem(parity + (s + dx + dy), 2)],
            dst_ref=a_recv.at[s, b],
            send_sem=a_ssem.at[0, s],
            recv_sem=a_rsem.at[0, s],
            device_id=(chip * 2 + core, g),
            device_id_type=MESH,
        )

    def send_a():
        for s in range(2):
            for dx, dy in A_ORDER:
                for dc in range(2):
                    a_copy(s, dx, dy, dc).start()
            a_copy(s, 0, 0, 1).start()
            a_recv[s, b] = a_send[q, c * 2 + lax.rem(parity + s, 2)]

    def swap(p):
        return pltpu.make_async_remote_copy(
            src_ref=d_send.at[p - 1],
            dst_ref=d_recv.at[p - 1],
            send_sem=d_ssem.at[p - 1],
            recv_sem=d_rsem.at[p - 1],
            device_id=(q * 2 + 1 - c, g),
            device_id_type=MESH,
        )

    def m_copy(p, s, dx, dy):
        chip = chip_at(dx, dy)
        return pltpu.make_async_remote_copy(
            src_ref=m_send.at[p - 1, chip, lax.rem(parity + (s + dx + dy), 2)],
            dst_ref=m_recv.at[p - 1, s, q],
            send_sem=a_ssem.at[p, s],
            recv_sem=a_rsem.at[p, s],
            device_id=(chip * 2 + c, g),
            device_id_type=MESH,
        )

    def send_m(p):
        swap(p).wait_recv()
        m_send[p - 1] = m_send[p - 1] + d_recv[p - 1]
        for s in range(2):
            for dx, dy in A_ORDER:
                m_copy(p, s, dx, dy).start()
            m_recv[p - 1, s, q] = m_send[p - 1, q, lax.rem(parity + s, 2)]

    def a_all(p, s):
        if p == 0:
            ref = a_recv.at[s, pl.ds(0, GROUPS - 1)]
        else:
            ref = m_recv.at[p - 1, s, pl.ds(0, CHIPS - 1)]
        return pltpu.make_async_remote_copy(
            src_ref=ref,
            dst_ref=ref,
            send_sem=a_ssem.at[p, s],
            recv_sem=a_rsem.at[p, s],
            device_id=(b, g),
            device_id_type=MESH,
        )

    with jax.named_scope("sums#p=0"):
        partial_sums(0, mixing, store_groups)
    with jax.named_scope("barrier"):
        pl.semaphore_wait(barrier, greeted)
    with jax.named_scope("send_a#p=0"):
        send_a()
    mixing = chip_mixing()
    for p in range(1, PHASES):
        with jax.named_scope(f"sums#p={p}"):
            partial_sums(p, mixing, store_chips(p))
        swap(p).start()
    for p in range(1, PHASES):
        with jax.named_scope(f"send_m#p={p}"):
            send_m(p)

    def source_rows(per_source, used, bands):
        source = iota((1, GROUPS * ROWS), 1)
        local = source & (per_source - 1)
        slot = (local * 11) >> 5
        t = jnp.where(local < used, local - slot * TRI, -1)
        first = ((source // per_source) * bands).astype(F32)
        begun = jnp.sum(jnp.where(ends <= first, 1.0, 0.0), axis=0, keepdims=True)
        return begun + slot.astype(F32), t

    sources = (
        (select, source_rows(ROWS, USED, BANDS)),
        (chip_select, source_rows(CHIP_ROWS, CHIP_USED, 2 * BANDS)),
    )
    block = OUT // 4
    for e in range(4):
        in_slot, cc = e >> 1, e & 1
        r = iota((block, NSLICE), 0)
        place = (((r * 43) >> 7) * 2 + cc) * 2 + in_slot
        lane = iota((block, NSLICE), 1)
        target = jnp.sum(jnp.where(lane == place, owner_row, 0.0), axis=1, keepdims=True)
        bands = jnp.sum(
            jnp.where(lane.astype(F32) == target, width_row, 0.0), axis=1, keepdims=True
        )
        scale[e * block : (e + 1) * block, :] = jnp.broadcast_to(1.0 / jnp.sqrt(bands), (block, 128))
        r2 = iota((block, GROUPS * ROWS), 0)
        t2 = r2 - ((r2 * 43) >> 7) * TRI
        for matrix, (source_slice, source_t) in sources:
            hit = (target == source_slice) & (t2 == source_t)
            matrix[e * block : (e + 1) * block, :] = jnp.where(hit, 1.0, 0.0).astype(BF16)

    in_class = lax.rem(g, 4) // 2 == c

    def z_rows(s, e):
        return pl.ds((s * 4 + e) * CHIPS, CHIPS)

    def combine(p, s):
        with jax.named_scope(f"wait_a#p={p}#s={s}"):
            a_all(p, s).wait_recv()
        if p == 0:
            matrix, part, spare = select, a_recv[s], (GROUPS, ROWS - USED, 128)
        else:
            matrix, part, spare = chip_select, m_recv[p - 1, s], (CHIPS, CHIP_ROWS - CHIP_USED, 128)
        part = jnp.concatenate([part, jnp.zeros(spare, F32)], axis=1).reshape(GROUPS * ROWS, 128)
        high = part.astype(BF16)
        low = (part - high.astype(F32)).astype(BF16)
        both = jnp.dot(
            matrix[...], jnp.concatenate([high, low], axis=1), preferred_element_type=F32
        )
        rows = (both[:, :128] + both[:, 128:]) * scale[...]
        for e in range(4):
            z_send[p, z_rows(s, e)] = rows[e * block : (e + 1) * block].reshape(CHIPS, TRI, 128)

    def z_copy(p, s, e):
        plane = (e >> 1) * 4 + 2 * c + lax.rem(parity + s, 2)
        core = e & 1
        copy = pltpu.make_async_remote_copy(
            src_ref=z_send.at[p, z_rows(s, e)],
            dst_ref=z_recv.at[p, :, g],
            send_sem=z_ssem.at[p, s],
            recv_sem=b_rsem.at[PHASES + p],
            device_id=(q * 2 + core, plane),
            device_id_type=MESH,
        )
        here = (plane == g) & (core == c)
        return copy, here

    def send_z(p, s):
        for e in range(4):
            copy, here = z_copy(p, s, e)

            @pl.when(jnp.logical_not(here))
            def _():
                copy.start()

            @pl.when(here)
            def _():
                z_recv[p, :, g] = z_send[p, z_rows(s, e)]

    def blocks(p, s, count):
        return pltpu.make_async_remote_copy(
            src_ref=z_send.at[p, pl.ds(0, count)],
            dst_ref=z_send.at[p, pl.ds(0, count)],
            send_sem=z_ssem.at[p, s],
            recv_sem=b_rsem.at[PHASES + p],
            device_id=(b, g),
            device_id_type=MESH,
        )

    def wait_z(p):
        @pl.when(in_class)
        def _():
            blocks(p, 0, (NZ - 1) * CHIPS).wait_recv()

        @pl.when(jnp.logical_not(in_class))
        def _():
            blocks(p, 0, NZ * CHIPS).wait_recv()

    def b_copy(p, dx, dy):
        chip = chip_at(dx, dy)
        return pltpu.make_async_remote_copy(
            src_ref=z_recv.at[p, chip],
            dst_ref=out_ref.at[:, p, q],
            send_sem=b_ssem.at[p],
            recv_sem=b_rsem.at[p],
            device_id=(chip * 2 + c, g),
            device_id_type=MESH,
        )

    def b_all(p):
        return pltpu.make_async_remote_copy(
            src_ref=z_recv.at[p, pl.ds(0, CHIPS - 1)],
            dst_ref=z_recv.at[p, pl.ds(0, CHIPS - 1)],
            send_sem=b_ssem.at[p],
            recv_sem=b_rsem.at[p],
            device_id=(b, g),
            device_id_type=MESH,
        )

    def d_copy(p, s, e, dx, dy):
        plane = (e >> 1) * 4 + 2 * c + lax.rem(parity + s, 2)
        core = e & 1
        chip = chip_at(dx, dy)
        copy = pltpu.make_async_remote_copy(
            src_ref=z_send.at[p, (s * 4 + e) * CHIPS + chip],
            dst_ref=out_ref.at[g, p, q],
            send_sem=z_ssem.at[p, s],
            recv_sem=b_rsem.at[p],
            device_id=(chip * 2 + core, plane),
            device_id_type=MESH,
        )
        return copy, (plane == g) & (core == c)

    def send_d(p, s):
        for dx, dy in tuple(reversed(OFFSETS)):
            for e in range(4):
                d_copy(p, s, e, dx, dy)[0].start()
        for e in range(4):
            copy, here = d_copy(p, s, e, 0, 0)

            @pl.when(jnp.logical_not(here))
            def _():
                copy.start()

            @pl.when(here)
            def _():
                out_ref[g, p, q] = z_send[p, (s * 4 + e) * CHIPS + q]

    def d_all(p, s, count):
        return pltpu.make_async_remote_copy(
            src_ref=z_send.at[p, pl.ds(0, count)],
            dst_ref=z_send.at[p, pl.ds(0, count)],
            send_sem=z_ssem.at[p, s],
            recv_sem=b_rsem.at[p],
            device_id=(b, g),
            device_id_type=MESH,
        )

    mine = lax.rem(g + parity, 2)

    def pass_on(p, s):
        @pl.when(mine == s)
        def _():
            with jax.named_scope(f"wait_z#p={p}#s={s}"):
                wait_z(p)
            for dx, dy in reversed(OFFSETS):
                b_copy(p, dx, dy).start()
            out_ref[:, p, q] = z_recv[p, q]

    steps = [(p, s) for p in range(PHASES) for s in range(2)]
    for k, step in enumerate(steps):
        combine(*step)
        with jax.named_scope(f"send_z#p={step[0]}#s={step[1]}"):
            (send_d if step in DIRECT else send_z)(*step)
        if k >= LAG and steps[k - LAG] not in DIRECT:
            pass_on(*steps[k - LAG])
    for step in steps[-LAG:]:
        if step not in DIRECT:
            pass_on(*step)

    for p in range(PHASES):
        for s in range(2):
            a_all(p, s).wait_send()
            own = in_class & (mine == s)
            part = 1 if (p, s) in DIRECT else CHIPS

            @pl.when(own)
            def _():
                blocks(p, s, 4 * CHIPS - part).wait_send()

            @pl.when(jnp.logical_not(own))
            def _():
                blocks(p, s, 4 * CHIPS).wait_send()

    for p in range(1, PHASES):
        swap(p).wait_send()

    for p in range(PHASES):
        for s in range(2):

            @pl.when(mine == s)
            def _():
                with jax.named_scope(f"wait_b#p={p}#s={s}"):
                    if (p, s) in DIRECT:

                        @pl.when(in_class)
                        def _():
                            d_all(p, s, NZ * CHIPS - 1).wait_recv()

                        @pl.when(jnp.logical_not(in_class))
                        def _():
                            d_all(p, s, NZ * CHIPS).wait_recv()

                    else:
                        b_all(p).wait_recv()
                        b_all(p).wait_send()


def on_device(band_coeffs, sign_table, slice_widths, owner_map):
    hbm = pl.BlockSpec(memory_space=pltpu.HBM)
    operands = (band_coeffs, sign_table, slice_widths.reshape(1, NSLICE), owner_map.reshape(1, NSLICE))
    operands = [pltpu.with_memory_space_constraint(v, pltpu.HBM) for v in operands]
    rows = pl.pallas_call(
        kernel,
        out_shape=jax.ShapeDtypeStruct((NZ, PHASES, CHIPS, TRI, 128), F32),
        in_specs=[hbm] * 4,
        out_specs=pl.BlockSpec(memory_space=pltpu.VMEM),
        scratch_shapes=[
            pltpu.VMEM((PHASES, BANDS, WIDE), F32),
            pltpu.VMEM((NPS, BANDS), jnp.int32),
            pltpu.VMEM((1, NSLICE), jnp.int32),
            pltpu.VMEM((1, NSLICE), jnp.int32),
            pltpu.VMEM((OUT, GROUPS * ROWS), BF16),
            pltpu.VMEM((OUT, GROUPS * ROWS), BF16),
            pltpu.VMEM((OUT, 128), F32),
            pltpu.VMEM((CHIPS, 4, USED, 128), F32),
            pltpu.VMEM((2, GROUPS, USED, 128), F32),
            pltpu.VMEM((PHASES - 1, CHIPS, 2, CHIP_USED, 128), F32),
            pltpu.VMEM((PHASES - 1, CHIPS, 2, CHIP_USED, 128), F32),
            pltpu.VMEM((PHASES - 1, CHIPS, 2, CHIP_USED, 128), F32),
            pltpu.VMEM((PHASES - 1, 2, CHIPS, CHIP_USED, 128), F32),
            pltpu.VMEM((PHASES, 2 * 4 * CHIPS, TRI, 128), F32),
            pltpu.VMEM((PHASES, CHIPS, NZ, TRI, 128), F32),
            pltpu.SemaphoreType.DMA((PHASES,)),
            pltpu.SemaphoreType.DMA((3,)),
            pltpu.SemaphoreType.DMA((PHASES, 2)),
            pltpu.SemaphoreType.DMA((PHASES, 2)),
            pltpu.SemaphoreType.DMA((PHASES - 1,)),
            pltpu.SemaphoreType.DMA((PHASES - 1,)),
            pltpu.SemaphoreType.DMA((PHASES, 2)),
            pltpu.SemaphoreType.DMA((PHASES,)),
            pltpu.SemaphoreType.DMA((2 * PHASES,)),
        ],
        compiler_params=pltpu.CompilerParams(
            collective_id=0, has_side_effects=True, vmem_limit_bytes=VMEM_LIMIT
        ),
        name="pseudobands",
    )(*operands)
    return jnp.transpose(rows.reshape(-1, TRI, 128), (1, 0, 2)).reshape(TRI, NZ * SLAB)


def solution(mesh):
    return jax.shard_map(
        on_device,
        mesh=mesh,
        in_specs=(P("band", "gslab"), P(None, "band"), P(), P()),
        out_specs=P(("band", "gslab"), None),
        check_vma=False,
    )
```

```python
import jax
import jax.numpy as jnp
from jax import lax
from jax.experimental import pallas as pl
from jax.experimental.pallas import tpu as pltpu
from jax.sharding import PartitionSpec as P

MESH = pl.DeviceIdType.MESH
F32 = jnp.float32
BF16 = jnp.bfloat16

NX, NY, NZ = 4, 4, 8
CHIPS = NX * NY
GROUPS = 2 * CHIPS
BANDS = 384
SLAB = 6144
PHASES = 3
WIDE = SLAB // PHASES
NPS = 12
TRI = 3
SLOTS = 5
ROWS = 16
USED = SLOTS * TRI
CHIP_SLOTS = 9
CHIP_ROWS = 32
CHIP_USED = CHIP_SLOTS * TRI
NSLICE = 64
OUT = NSLICE * TRI
LAG = 2
VMEM_LIMIT = 52 * 10**6

OFFSETS = (
    (1, 0), (0, 1), (3, 0), (0, 3), (1, 1), (3, 3), (1, 3), (3, 1),
    (2, 0), (0, 2), (2, 1), (1, 2), (2, 3), (3, 2), (2, 2),
)

A_ORDER = ((2, 2), (2, 1), (2, 3), (2, 0), (1, 2), (3, 2), (1, 1), (3, 3), (1, 3), (3, 1), (1, 0), (3, 0), (0, 2), (0, 1), (0, 3))


def iota(shape, dim):
    return lax.broadcasted_iota(jnp.int32, shape, dim)


def kernel(
    band_ref, sign_ref, width_ref, owner_ref, out_ref,
    coeffs, sign, width, owner, select, chip_select, scale,
    a_send, a_recv, d_send, d_recv, m_send, m_recv, z_send, z_recv,
    load_sem, small_sem, a_ssem, a_rsem, d_ssem, d_rsem, z_ssem, b_ssem, b_rsem,
):
    b = lax.axis_index("band")
    g = lax.axis_index("gslab")
    c = lax.rem(b, 2)
    q = b // 2
    x = lax.rem(q, NX)
    y = q // NX
    parity = lax.rem(x + y, 2)

    ring = lax.rem(g - 2 * c + NZ, 4)
    last = 1 - lax.rem((ring + 1) // 2, 2)

    def triple(p, s, shift=0):
        return lax.rem(last + 1 + s, 2) if p == PHASES - 1 else lax.rem(parity + (s + shift), 2)

    def chip_at(dx, dy):
        return lax.rem(y + dy, NY) * NX + lax.rem(x + dx, NX)

    loads = [
        pltpu.make_async_copy(band_ref.at[:, pl.ds(p * WIDE, WIDE)], coeffs.at[p], load_sem.at[p])
        for p in range(PHASES)
    ]
    smalls = [
        pltpu.make_async_copy(src, dst, small_sem.at[i])
        for i, (src, dst) in enumerate(((sign_ref, sign), (width_ref, width), (owner_ref, owner)))
    ]
    for copy in smalls:
        copy.start()
    loads[0].start()

    barrier = pltpu.get_barrier_semaphore()
    greeted = 0
    for dx, dy in reversed(OFFSETS):
        for core in range(2):
            pl.semaphore_signal(
                barrier, inc=1, device_id=(chip_at(dx, dy) * 2 + core, g), device_id_type=MESH
            )
            greeted += 1
    pl.semaphore_signal(barrier, inc=1, device_id=(q * 2 + 1 - c, g), device_id_type=MESH)
    greeted += 1
    for dz in (4, 3, 5, 2, 6, 1, 7):
        for core in range(2):
            pl.semaphore_signal(
                barrier, inc=1, device_id=(q * 2 + core, lax.rem(g + dz, NZ)), device_id_type=MESH
            )
            greeted += 1
    for copy in loads[1:]:
        copy.start()

    for copy in smalls:
        copy.wait()
    width_row = width[...].astype(F32)
    owner_row = owner[...].astype(F32)
    ends = jnp.sum(
        jnp.where(iota((NSLICE, NSLICE), 1) <= iota((NSLICE, NSLICE), 0), width_row, 0.0),
        axis=1, keepdims=True,
    )
    first = b * BANDS
    band_row = (first + iota((1, BANDS), 1)).astype(F32)
    slice_row = jnp.sum(jnp.where(ends <= band_row, 1.0, 0.0), axis=0, keepdims=True)
    first_row = jnp.zeros((1, BANDS), F32) + first.astype(F32)
    first_slice = jnp.sum(jnp.where(ends <= first_row, 1.0, 0.0), axis=0, keepdims=True)
    row = iota((4 * ROWS, BANDS), 0)
    local = row & (ROWS - 1)
    slot = (local * 11) >> 5
    pseudo = (row >> 4) * TRI + local - slot * TRI
    sign_f = sign[...].astype(F32)
    signs = jnp.zeros((4 * ROWS, BANDS), F32)
    for j in range(NPS):
        signs = jnp.where(pseudo == j, sign_f[j : j + 1, :], signs)
    member = (slice_row - first_slice == slot.astype(F32)) & (local < SLOTS * TRI)
    mixing = jnp.where(member, signs, 0.0).astype(BF16)
    mixing = jnp.concatenate([mixing, mixing], axis=1)

    def chip_mixing():
        row = iota((4 * CHIP_ROWS, BANDS), 0)
        local = row & (CHIP_ROWS - 1)
        slot = (local * 11) >> 5
        half = jnp.where(row < 2 * CHIP_ROWS, c, 1 - c)
        pseudo = (half * 2 + ((row >> 5) & 1)) * TRI + local - slot * TRI
        signs = jnp.zeros((4 * CHIP_ROWS, BANDS), F32)
        for j in range(NPS):
            signs = jnp.where(pseudo == j, sign_f[j : j + 1, :], signs)
        chip_row = jnp.zeros((1, BANDS), F32) + (q * (2 * BANDS)).astype(F32)
        chip_slice = jnp.sum(jnp.where(ends <= chip_row, 1.0, 0.0), axis=0, keepdims=True)
        member = (slice_row - chip_slice == slot.astype(F32)) & (local < CHIP_USED)
        mixing = jnp.where(member, signs, 0.0).astype(BF16)
        return jnp.concatenate([mixing, mixing], axis=1)

    def partial_sums(p, mixing, store):
        loads[p].wait()

        @pl.loop(0, CHIPS // 2, unroll=4)
        def _(pair):
            part = coeffs[p, :, pl.ds(pl.multiple_of(pair * 256, 256), 256)]
            high = part.astype(BF16)
            low = (part - high.astype(F32)).astype(BF16)
            sums = jnp.dot(
                mixing, jnp.concatenate([high, low], axis=0), preferred_element_type=F32
            )
            for side in range(2):
                store(pair * 2 + side, sums[:, side * 128 : (side + 1) * 128])

    def store_groups(chip, sums):
        for part in range(4):
            a_send[chip, part] = sums[part * ROWS : part * ROWS + USED]

    def store_chips(p):
        def store(chip, sums):
            for h in range(2):
                own = h * CHIP_ROWS
                m_send[p - 1, chip, h] = sums[own : own + CHIP_USED]
                other = own + 2 * CHIP_ROWS
                d_send[p - 1, chip, h] = sums[other : other + CHIP_USED]

        return store

    def a_copy(s, dx, dy, dc):
        chip = chip_at(dx, dy)
        core = lax.rem(c + dc, 2)
        return pltpu.make_async_remote_copy(
            src_ref=a_send.at[chip, core * 2 + triple(0, s, dx + dy)],
            dst_ref=a_recv.at[s, b],
            send_sem=a_ssem.at[0, s],
            recv_sem=a_rsem.at[0, s],
            device_id=(chip * 2 + core, g),
            device_id_type=MESH,
        )

    def send_a():
        for s in range(2):
            for dx, dy in A_ORDER:
                for dc in range(2):
                    a_copy(s, dx, dy, dc).start()
            a_copy(s, 0, 0, 1).start()
            a_recv[s, b] = a_send[q, c * 2 + triple(0, s)]

    def swap(p):
        return pltpu.make_async_remote_copy(
            src_ref=d_send.at[p - 1],
            dst_ref=d_recv.at[p - 1],
            send_sem=d_ssem.at[p - 1],
            recv_sem=d_rsem.at[p - 1],
            device_id=(q * 2 + 1 - c, g),
            device_id_type=MESH,
        )

    def m_copy(p, s, dx, dy):
        chip = chip_at(dx, dy)
        return pltpu.make_async_remote_copy(
            src_ref=m_send.at[p - 1, chip, triple(p, s, dx + dy)],
            dst_ref=m_recv.at[p - 1, s, q],
            send_sem=a_ssem.at[p, s],
            recv_sem=a_rsem.at[p, s],
            device_id=(chip * 2 + c, g),
            device_id_type=MESH,
        )

    def send_m(p):
        swap(p).wait_recv()
        m_send[p - 1] = m_send[p - 1] + d_recv[p - 1]
        for s in range(2):
            for dx, dy in A_ORDER:
                m_copy(p, s, dx, dy).start()
            m_recv[p - 1, s, q] = m_send[p - 1, q, triple(p, s)]

    def a_all(p, s):
        if p == 0:
            ref = a_recv.at[s, pl.ds(0, GROUPS - 1)]
        else:
            ref = m_recv.at[p - 1, s, pl.ds(0, CHIPS - 1)]
        return pltpu.make_async_remote_copy(
            src_ref=ref,
            dst_ref=ref,
            send_sem=a_ssem.at[p, s],
            recv_sem=a_rsem.at[p, s],
            device_id=(b, g),
            device_id_type=MESH,
        )

    with jax.named_scope("sums#p=0"):
        partial_sums(0, mixing, store_groups)
    with jax.named_scope("barrier"):
        pl.semaphore_wait(barrier, greeted)
    with jax.named_scope("send_a#p=0"):
        send_a()
    mixing = chip_mixing()
    for p in range(1, PHASES):
        with jax.named_scope(f"sums#p={p}"):
            partial_sums(p, mixing, store_chips(p))
        swap(p).start()
    for p in range(1, PHASES):
        with jax.named_scope(f"send_m#p={p}"):
            send_m(p)

    def source_rows(per_source, used, bands):
        source = iota((1, GROUPS * ROWS), 1)
        local = source & (per_source - 1)
        slot = (local * 11) >> 5
        t = jnp.where(local < used, local - slot * TRI, -1)
        first = ((source // per_source) * bands).astype(F32)
        begun = jnp.sum(jnp.where(ends <= first, 1.0, 0.0), axis=0, keepdims=True)
        return begun + slot.astype(F32), t

    sources = (
        (select, source_rows(ROWS, USED, BANDS)),
        (chip_select, source_rows(CHIP_ROWS, CHIP_USED, 2 * BANDS)),
    )
    block = OUT // 4
    for e in range(4):
        in_slot, cc = e >> 1, e & 1
        r = iota((block, NSLICE), 0)
        place = (((r * 43) >> 7) * 2 + cc) * 2 + in_slot
        lane = iota((block, NSLICE), 1)
        target = jnp.sum(jnp.where(lane == place, owner_row, 0.0), axis=1, keepdims=True)
        bands = jnp.sum(
            jnp.where(lane.astype(F32) == target, width_row, 0.0), axis=1, keepdims=True
        )
        scale[e * block : (e + 1) * block, :] = jnp.broadcast_to(1.0 / jnp.sqrt(bands), (block, 128))
        r2 = iota((block, GROUPS * ROWS), 0)
        t2 = r2 - ((r2 * 43) >> 7) * TRI
        for matrix, (source_slice, source_t) in sources:
            hit = (target == source_slice) & (t2 == source_t)
            matrix[e * block : (e + 1) * block, :] = jnp.where(hit, 1.0, 0.0).astype(BF16)

    in_class = lax.rem(g, 4) // 2 == c

    def z_rows(s, e):
        return pl.ds((s * 4 + e) * CHIPS, CHIPS)

    def combine(p, s):
        with jax.named_scope(f"wait_a#p={p}#s={s}"):
            a_all(p, s).wait_recv()
        if p == 0:
            matrix, part, spare = select, a_recv[s], (GROUPS, ROWS - USED, 128)
        else:
            matrix, part, spare = chip_select, m_recv[p - 1, s], (CHIPS, CHIP_ROWS - CHIP_USED, 128)
        part = jnp.concatenate([part, jnp.zeros(spare, F32)], axis=1).reshape(GROUPS * ROWS, 128)
        high = part.astype(BF16)
        low = (part - high.astype(F32)).astype(BF16)
        both = jnp.dot(
            matrix[...], jnp.concatenate([high, low], axis=1), preferred_element_type=F32
        )
        rows = (both[:, :128] + both[:, 128:]) * scale[...]
        for e in range(4):
            z_send[p, z_rows(s, e)] = rows[e * block : (e + 1) * block].reshape(CHIPS, TRI, 128)

    def z_copy(p, s, e):
        plane = (e >> 1) * 4 + 2 * c + triple(p, s)
        core = e & 1
        copy = pltpu.make_async_remote_copy(
            src_ref=z_send.at[p, z_rows(s, e)],
            dst_ref=z_recv.at[p, :, g],
            send_sem=z_ssem.at[p, s],
            recv_sem=b_rsem.at[PHASES + p],
            device_id=(q * 2 + core, plane),
            device_id_type=MESH,
        )
        here = (plane == g) & (core == c)
        return copy, here

    def send_z(p, s):
        for e in range(4):
            copy, here = z_copy(p, s, e)

            @pl.when(jnp.logical_not(here))
            def _():
                copy.start()

            @pl.when(here)
            def _():
                z_recv[p, :, g] = z_send[p, z_rows(s, e)]

    def blocks(p, s, count):
        return pltpu.make_async_remote_copy(
            src_ref=z_send.at[p, pl.ds(0, count)],
            dst_ref=z_send.at[p, pl.ds(0, count)],
            send_sem=z_ssem.at[p, s],
            recv_sem=b_rsem.at[PHASES + p],
            device_id=(b, g),
            device_id_type=MESH,
        )

    def wait_z(p):
        @pl.when(in_class)
        def _():
            blocks(p, 0, (NZ - 1) * CHIPS).wait_recv()

        @pl.when(jnp.logical_not(in_class))
        def _():
            blocks(p, 0, NZ * CHIPS).wait_recv()

    def b_copy(p, dx, dy):
        chip = chip_at(dx, dy)
        return pltpu.make_async_remote_copy(
            src_ref=z_recv.at[p, chip],
            dst_ref=out_ref.at[:, p, q],
            send_sem=b_ssem.at[p],
            recv_sem=b_rsem.at[p],
            device_id=(chip * 2 + c, g),
            device_id_type=MESH,
        )

    def b_all(p):
        return pltpu.make_async_remote_copy(
            src_ref=z_recv.at[p, pl.ds(0, CHIPS - 1)],
            dst_ref=z_recv.at[p, pl.ds(0, CHIPS - 1)],
            send_sem=b_ssem.at[p],
            recv_sem=b_rsem.at[p],
            device_id=(b, g),
            device_id_type=MESH,
        )

    def d_copy(p, s, order, core, dx, dy):
        first = 2 * c + triple(p, s)
        away = lax.rem(g - first + NZ, NZ)
        far = jnp.where((away >= 2) & (away <= 6), 0, 1)
        upper = lax.rem(far + order, 2)
        chip = chip_at(dx, dy)
        row = (s * 4 + upper * 2 + core) * CHIPS + chip
        plane = upper * 4 + first
        copy = pltpu.make_async_remote_copy(
            src_ref=z_send.at[p, row],
            dst_ref=out_ref.at[g, p, q],
            send_sem=z_ssem.at[p, s],
            recv_sem=b_rsem.at[p],
            device_id=(chip * 2 + core, plane),
            device_id_type=MESH,
        )
        return copy, row, (plane == g) & (core == c)

    def send_d(p, s):
        for order in range(2):
            for dx, dy in A_ORDER:
                for core in range(2):
                    d_copy(p, s, order, core, dx, dy)[0].start()
            for core in range(2):
                copy, row, here = d_copy(p, s, order, core, 0, 0)

                @pl.when(jnp.logical_not(here))
                def _():
                    copy.start()

                @pl.when(here)
                def _():
                    out_ref[g, p, q] = z_send[p, row]

    def d_all(p, count):
        return pltpu.make_async_remote_copy(
            src_ref=z_send.at[p, pl.ds(0, count)],
            dst_ref=z_send.at[p, pl.ds(0, count)],
            send_sem=z_ssem.at[p, 0],
            recv_sem=b_rsem.at[p],
            device_id=(b, g),
            device_id_type=MESH,
        )

    mine = lax.rem(g + parity, 2)

    def pass_on(p, s):
        @pl.when(mine == s)
        def _():
            with jax.named_scope(f"wait_z#p={p}#s={s}"):
                wait_z(p)
            for dx, dy in A_ORDER:
                b_copy(p, dx, dy).start()
            out_ref[:, p, q] = z_recv[p, q]

    final = PHASES - 1
    steps = [(p, s) for p in range(PHASES) for s in range(2)]
    for k, (p, s) in enumerate(steps):
        combine(p, s)
        with jax.named_scope(f"send_z#p={p}#s={s}"):
            if p < final:
                send_z(p, s)
            else:
                send_d(p, s)
        if k >= LAG:
            pass_on(*steps[k - LAG])

    for p, s in steps:
        a_all(p, s).wait_send()
        own = in_class & ((mine == s) if p < final else (s == 0))
        part = CHIPS if p < final else 1

        @pl.when(own)
        def _():
            blocks(p, s, 4 * CHIPS - part).wait_send()

        @pl.when(jnp.logical_not(own))
        def _():
            blocks(p, s, 4 * CHIPS).wait_send()

    for p in range(1, PHASES):
        swap(p).wait_send()
    for p in range(final):
        with jax.named_scope(f"wait_b#p={p}"):
            b_all(p).wait_recv()
            b_all(p).wait_send()
    with jax.named_scope("wait_d"):

        @pl.when(in_class)
        def _():
            d_all(final, NZ * CHIPS - 1).wait_recv()

        @pl.when(jnp.logical_not(in_class))
        def _():
            d_all(final, NZ * CHIPS).wait_recv()


def on_device(band_coeffs, sign_table, slice_widths, owner_map):
    hbm = pl.BlockSpec(memory_space=pltpu.HBM)
    operands = (band_coeffs, sign_table, slice_widths.reshape(1, NSLICE), owner_map.reshape(1, NSLICE))
    operands = [pltpu.with_memory_space_constraint(v, pltpu.HBM) for v in operands]
    rows = pl.pallas_call(
        kernel,
        out_shape=jax.ShapeDtypeStruct((NZ, PHASES, CHIPS, TRI, 128), F32),
        in_specs=[hbm] * 4,
        out_specs=pl.BlockSpec(memory_space=pltpu.VMEM),
        scratch_shapes=[
            pltpu.VMEM((PHASES, BANDS, WIDE), F32),
            pltpu.VMEM((NPS, BANDS), jnp.int32),
            pltpu.VMEM((1, NSLICE), jnp.int32),
            pltpu.VMEM((1, NSLICE), jnp.int32),
            pltpu.VMEM((OUT, GROUPS * ROWS), BF16),
            pltpu.VMEM((OUT, GROUPS * ROWS), BF16),
            pltpu.VMEM((OUT, 128), F32),
            pltpu.VMEM((CHIPS, 4, USED, 128), F32),
            pltpu.VMEM((2, GROUPS, USED, 128), F32),
            pltpu.VMEM((PHASES - 1, CHIPS, 2, CHIP_USED, 128), F32),
            pltpu.VMEM((PHASES - 1, CHIPS, 2, CHIP_USED, 128), F32),
            pltpu.VMEM((PHASES - 1, CHIPS, 2, CHIP_USED, 128), F32),
            pltpu.VMEM((PHASES - 1, 2, CHIPS, CHIP_USED, 128), F32),
            pltpu.VMEM((PHASES, 2 * 4 * CHIPS, TRI, 128), F32),
            pltpu.VMEM((PHASES, CHIPS, NZ, TRI, 128), F32),
            pltpu.SemaphoreType.DMA((PHASES,)),
            pltpu.SemaphoreType.DMA((3,)),
            pltpu.SemaphoreType.DMA((PHASES, 2)),
            pltpu.SemaphoreType.DMA((PHASES, 2)),
            pltpu.SemaphoreType.DMA((PHASES - 1,)),
            pltpu.SemaphoreType.DMA((PHASES - 1,)),
            pltpu.SemaphoreType.DMA((PHASES, 2)),
            pltpu.SemaphoreType.DMA((PHASES,)),
            pltpu.SemaphoreType.DMA((2 * PHASES,)),
        ],
        compiler_params=pltpu.CompilerParams(
            collective_id=0, has_side_effects=True, vmem_limit_bytes=VMEM_LIMIT
        ),
        name="pseudobands",
    )(*operands)
    return jnp.transpose(rows.reshape(-1, TRI, 128), (1, 0, 2)).reshape(TRI, NZ * SLAB)


def solution(mesh):
    return jax.shard_map(
        on_device,
        mesh=mesh,
        in_specs=(P("band", "gslab"), P(None, "band"), P(), P()),
        out_specs=P(("band", "gslab"), None),
        check_vma=False,
    )
```

```python
import jax
import jax.numpy as jnp
from jax import lax
from jax.experimental import pallas as pl
from jax.experimental.pallas import tpu as pltpu
from jax.sharding import PartitionSpec as P

MESH = pl.DeviceIdType.MESH
F32 = jnp.float32
BF16 = jnp.bfloat16

NX, NY, NZ = 4, 4, 8
CHIPS = NX * NY
GROUPS = 2 * CHIPS
BANDS = 384
SLAB = 6144
PHASES = 3
WIDE = SLAB // PHASES
NPS = 12
TRI = 3
SLOTS = 5
ROWS = 16
USED = SLOTS * TRI
CHIP_SLOTS = 9
CHIP_ROWS = 32
CHIP_USED = CHIP_SLOTS * TRI
NSLICE = 64
OUT = NSLICE * TRI
LAG = 2
VMEM_LIMIT = 52 * 10**6

OFFSETS = (
    (1, 0), (0, 1), (3, 0), (0, 3), (1, 1), (3, 3), (1, 3), (3, 1),
    (2, 0), (0, 2), (2, 1), (1, 2), (2, 3), (3, 2), (2, 2),
)

A_ORDER = ((2, 2), (2, 1), (2, 3), (2, 0), (1, 2), (3, 2), (1, 1), (3, 3), (1, 3), (3, 1), (1, 0), (3, 0), (0, 2), (0, 1), (0, 3))


def iota(shape, dim):
    return lax.broadcasted_iota(jnp.int32, shape, dim)


def kernel(
    band_ref, sign_ref, width_ref, owner_ref, out_ref,
    coeffs, sign, width, owner, select, chip_select, scale,
    a_send, a_recv, d_send, d_recv, m_send, m_recv, z_send, z_recv,
    load_sem, small_sem, a_ssem, a_rsem, d_ssem, d_rsem, z_ssem, b_ssem, b_rsem,
):
    b = lax.axis_index("band")
    g = lax.axis_index("gslab")
    c = lax.rem(b, 2)
    q = b // 2
    x = lax.rem(q, NX)
    y = q // NX
    parity = lax.rem(x + y, 2)

    ring = lax.rem(g - 2 * c + NZ, 4)
    last = 1 - lax.rem((ring + 1) // 2, 2)

    def triple(p, s, shift=0):
        return lax.rem(last + 1 + s, 2) if p == PHASES - 1 else lax.rem(parity + (s + shift), 2)

    def chip_at(dx, dy):
        return lax.rem(y + dy, NY) * NX + lax.rem(x + dx, NX)

    loads = [
        pltpu.make_async_copy(band_ref.at[:, pl.ds(p * WIDE, WIDE)], coeffs.at[p], load_sem.at[p])
        for p in range(PHASES)
    ]
    smalls = [
        pltpu.make_async_copy(src, dst, small_sem.at[i])
        for i, (src, dst) in enumerate(((sign_ref, sign), (width_ref, width), (owner_ref, owner)))
    ]
    for copy in smalls:
        copy.start()
    loads[0].start()

    barrier = pltpu.get_barrier_semaphore()
    greeted = 0
    for dx, dy in reversed(OFFSETS):
        for core in range(2):
            pl.semaphore_signal(
                barrier, inc=1, device_id=(chip_at(dx, dy) * 2 + core, g), device_id_type=MESH
            )
            greeted += 1
    pl.semaphore_signal(barrier, inc=1, device_id=(q * 2 + 1 - c, g), device_id_type=MESH)
    greeted += 1
    for dz in (4, 3, 5, 2, 6, 1, 7):
        for core in range(2):
            pl.semaphore_signal(
                barrier, inc=1, device_id=(q * 2 + core, lax.rem(g + dz, NZ)), device_id_type=MESH
            )
            greeted += 1
    for copy in loads[1:]:
        copy.start()

    for copy in smalls:
        copy.wait()
    width_row = width[...].astype(F32)
    owner_row = owner[...].astype(F32)
    ends = jnp.sum(
        jnp.where(iota((NSLICE, NSLICE), 1) <= iota((NSLICE, NSLICE), 0), width_row, 0.0),
        axis=1, keepdims=True,
    )
    first = b * BANDS
    band_row = (first + iota((1, BANDS), 1)).astype(F32)
    slice_row = jnp.sum(jnp.where(ends <= band_row, 1.0, 0.0), axis=0, keepdims=True)
    first_row = jnp.zeros((1, BANDS), F32) + first.astype(F32)
    first_slice = jnp.sum(jnp.where(ends <= first_row, 1.0, 0.0), axis=0, keepdims=True)
    row = iota((4 * ROWS, BANDS), 0)
    local = row & (ROWS - 1)
    slot = (local * 11) >> 5
    pseudo = (row >> 4) * TRI + local - slot * TRI
    sign_f = sign[...].astype(F32)
    signs = jnp.zeros((4 * ROWS, BANDS), F32)
    for j in range(NPS):
        signs = jnp.where(pseudo == j, sign_f[j : j + 1, :], signs)
    member = (slice_row - first_slice == slot.astype(F32)) & (local < SLOTS * TRI)
    mixing = jnp.where(member, signs, 0.0).astype(BF16)
    mixing = jnp.concatenate([mixing, mixing], axis=1)

    def chip_mixing():
        row = iota((4 * CHIP_ROWS, BANDS), 0)
        local = row & (CHIP_ROWS - 1)
        slot = (local * 11) >> 5
        half = jnp.where(row < 2 * CHIP_ROWS, c, 1 - c)
        pseudo = (half * 2 + ((row >> 5) & 1)) * TRI + local - slot * TRI
        signs = jnp.zeros((4 * CHIP_ROWS, BANDS), F32)
        for j in range(NPS):
            signs = jnp.where(pseudo == j, sign_f[j : j + 1, :], signs)
        chip_row = jnp.zeros((1, BANDS), F32) + (q * (2 * BANDS)).astype(F32)
        chip_slice = jnp.sum(jnp.where(ends <= chip_row, 1.0, 0.0), axis=0, keepdims=True)
        member = (slice_row - chip_slice == slot.astype(F32)) & (local < CHIP_USED)
        mixing = jnp.where(member, signs, 0.0).astype(BF16)
        return jnp.concatenate([mixing, mixing], axis=1)

    def partial_sums(p, mixing, store):
        loads[p].wait()

        @pl.loop(0, CHIPS // 2, unroll=4)
        def _(pair):
            part = coeffs[p, :, pl.ds(pl.multiple_of(pair * 256, 256), 256)]
            high = part.astype(BF16)
            low = (part - high.astype(F32)).astype(BF16)
            sums = jnp.dot(
                mixing, jnp.concatenate([high, low], axis=0), preferred_element_type=F32
            )
            for side in range(2):
                store(pair * 2 + side, sums[:, side * 128 : (side + 1) * 128])

    def store_groups(chip, sums):
        for part in range(4):
            a_send[chip, part] = sums[part * ROWS : part * ROWS + USED]

    def store_chips(p):
        def store(chip, sums):
            for h in range(2):
                own = h * CHIP_ROWS
                m_send[p - 1, chip, h] = sums[own : own + CHIP_USED]
                other = own + 2 * CHIP_ROWS
                d_send[p - 1, chip, h] = sums[other : other + CHIP_USED]

        return store

    def a_copy(s, dx, dy, dc):
        chip = chip_at(dx, dy)
        core = lax.rem(c + dc, 2)
        return pltpu.make_async_remote_copy(
            src_ref=a_send.at[chip, core * 2 + triple(0, s, dx + dy)],
            dst_ref=a_recv.at[s, b],
            send_sem=a_ssem.at[0, s],
            recv_sem=a_rsem.at[0, s],
            device_id=(chip * 2 + core, g),
            device_id_type=MESH,
        )

    def send_a():
        for s in range(2):
            for dc in (1, 0):
                for dx, dy in A_ORDER:
                    a_copy(s, dx, dy, dc).start()
            a_copy(s, 0, 0, 1).start()
            a_recv[s, b] = a_send[q, c * 2 + triple(0, s)]

    def swap(p):
        return pltpu.make_async_remote_copy(
            src_ref=d_send.at[p - 1],
            dst_ref=d_recv.at[p - 1],
            send_sem=d_ssem.at[p - 1],
            recv_sem=d_rsem.at[p - 1],
            device_id=(q * 2 + 1 - c, g),
            device_id_type=MESH,
        )

    def m_copy(p, s, dx, dy):
        chip = chip_at(dx, dy)
        return pltpu.make_async_remote_copy(
            src_ref=m_send.at[p - 1, chip, triple(p, s, dx + dy)],
            dst_ref=m_recv.at[p - 1, s, q],
            send_sem=a_ssem.at[p, s],
            recv_sem=a_rsem.at[p, s],
            device_id=(chip * 2 + c, g),
            device_id_type=MESH,
        )

    def send_m(p):
        swap(p).wait_recv()
        m_send[p - 1] = m_send[p - 1] + d_recv[p - 1]
        for s in range(2):
            for dx, dy in A_ORDER:
                m_copy(p, s, dx, dy).start()
            m_recv[p - 1, s, q] = m_send[p - 1, q, triple(p, s)]

    def a_all(p, s):
        if p == 0:
            ref = a_recv.at[s, pl.ds(0, GROUPS - 1)]
        else:
            ref = m_recv.at[p - 1, s, pl.ds(0, CHIPS - 1)]
        return pltpu.make_async_remote_copy(
            src_ref=ref,
            dst_ref=ref,
            send_sem=a_ssem.at[p, s],
            recv_sem=a_rsem.at[p, s],
            device_id=(b, g),
            device_id_type=MESH,
        )

    with jax.named_scope("sums#p=0"):
        partial_sums(0, mixing, store_groups)
    with jax.named_scope("barrier"):
        pl.semaphore_wait(barrier, greeted)
    with jax.named_scope("send_a#p=0"):
        send_a()
    mixing = chip_mixing()
    for p in range(1, PHASES):
        with jax.named_scope(f"sums#p={p}"):
            partial_sums(p, mixing, store_chips(p))
        swap(p).start()
    for p in range(1, PHASES):
        with jax.named_scope(f"send_m#p={p}"):
            send_m(p)

    def source_rows(per_source, used, bands):
        source = iota((1, GROUPS * ROWS), 1)
        local = source & (per_source - 1)
        slot = (local * 11) >> 5
        t = jnp.where(local < used, local - slot * TRI, -1)
        first = ((source // per_source) * bands).astype(F32)
        begun = jnp.sum(jnp.where(ends <= first, 1.0, 0.0), axis=0, keepdims=True)
        return begun + slot.astype(F32), t

    sources = (
        (select, source_rows(ROWS, USED, BANDS)),
        (chip_select, source_rows(CHIP_ROWS, CHIP_USED, 2 * BANDS)),
    )
    block = OUT // 4
    for e in range(4):
        in_slot, cc = e >> 1, e & 1
        r = iota((block, NSLICE), 0)
        place = (((r * 43) >> 7) * 2 + cc) * 2 + in_slot
        lane = iota((block, NSLICE), 1)
        target = jnp.sum(jnp.where(lane == place, owner_row, 0.0), axis=1, keepdims=True)
        bands = jnp.sum(
            jnp.where(lane.astype(F32) == target, width_row, 0.0), axis=1, keepdims=True
        )
        scale[e * block : (e + 1) * block, :] = jnp.broadcast_to(1.0 / jnp.sqrt(bands), (block, 128))
        r2 = iota((block, GROUPS * ROWS), 0)
        t2 = r2 - ((r2 * 43) >> 7) * TRI
        for matrix, (source_slice, source_t) in sources:
            hit = (target == source_slice) & (t2 == source_t)
            matrix[e * block : (e + 1) * block, :] = jnp.where(hit, 1.0, 0.0).astype(BF16)

    in_class = lax.rem(g, 4) // 2 == c

    def z_rows(s, e):
        return pl.ds((s * 4 + e) * CHIPS, CHIPS)

    def combine(p, s):
        with jax.named_scope(f"wait_a#p={p}#s={s}"):
            a_all(p, s).wait_recv()
        if p == 0:
            matrix, part, spare = select, a_recv[s], (GROUPS, ROWS - USED, 128)
        else:
            matrix, part, spare = chip_select, m_recv[p - 1, s], (CHIPS, CHIP_ROWS - CHIP_USED, 128)
        part = jnp.concatenate([part, jnp.zeros(spare, F32)], axis=1).reshape(GROUPS * ROWS, 128)
        high = part.astype(BF16)
        low = (part - high.astype(F32)).astype(BF16)
        both = jnp.dot(
            matrix[...], jnp.concatenate([high, low], axis=1), preferred_element_type=F32
        )
        rows = (both[:, :128] + both[:, 128:]) * scale[...]
        for e in range(4):
            z_send[p, z_rows(s, e)] = rows[e * block : (e + 1) * block].reshape(CHIPS, TRI, 128)

    def z_copy(p, s, e):
        plane = (e >> 1) * 4 + 2 * c + triple(p, s)
        core = e & 1
        copy = pltpu.make_async_remote_copy(
            src_ref=z_send.at[p, z_rows(s, e)],
            dst_ref=z_recv.at[p, :, g],
            send_sem=z_ssem.at[p, s],
            recv_sem=b_rsem.at[PHASES + p],
            device_id=(q * 2 + core, plane),
            device_id_type=MESH,
        )
        here = (plane == g) & (core == c)
        return copy, here

    def send_z(p, s):
        for e in range(4):
            copy, here = z_copy(p, s, e)

            @pl.when(jnp.logical_not(here))
            def _():
                copy.start()

            @pl.when(here)
            def _():
                z_recv[p, :, g] = z_send[p, z_rows(s, e)]

    def blocks(p, s, count):
        return pltpu.make_async_remote_copy(
            src_ref=z_send.at[p, pl.ds(0, count)],
            dst_ref=z_send.at[p, pl.ds(0, count)],
            send_sem=z_ssem.at[p, s],
            recv_sem=b_rsem.at[PHASES + p],
            device_id=(b, g),
            device_id_type=MESH,
        )

    def wait_z(p):
        @pl.when(in_class)
        def _():
            blocks(p, 0, (NZ - 1) * CHIPS).wait_recv()

        @pl.when(jnp.logical_not(in_class))
        def _():
            blocks(p, 0, NZ * CHIPS).wait_recv()

    def b_copy(p, dx, dy):
        chip = chip_at(dx, dy)
        return pltpu.make_async_remote_copy(
            src_ref=z_recv.at[p, chip],
            dst_ref=out_ref.at[:, p, q],
            send_sem=b_ssem.at[p],
            recv_sem=b_rsem.at[p],
            device_id=(chip * 2 + c, g),
            device_id_type=MESH,
        )

    def b_all(p):
        return pltpu.make_async_remote_copy(
            src_ref=z_recv.at[p, pl.ds(0, CHIPS - 1)],
            dst_ref=z_recv.at[p, pl.ds(0, CHIPS - 1)],
            send_sem=b_ssem.at[p],
            recv_sem=b_rsem.at[p],
            device_id=(b, g),
            device_id_type=MESH,
        )

    def d_copy(p, s, order, core, dx, dy):
        first = 2 * c + triple(p, s)
        away = lax.rem(g - first + NZ, NZ)
        far = jnp.where((away >= 2) & (away <= 6), 0, 1)
        upper = lax.rem(far + order, 2)
        chip = chip_at(dx, dy)
        row = (s * 4 + upper * 2 + core) * CHIPS + chip
        plane = upper * 4 + first
        copy = pltpu.make_async_remote_copy(
            src_ref=z_send.at[p, row],
            dst_ref=out_ref.at[g, p, q],
            send_sem=z_ssem.at[p, s],
            recv_sem=b_rsem.at[p],
            device_id=(chip * 2 + core, plane),
            device_id_type=MESH,
        )
        return copy, row, (plane == g) & (core == c)

    def send_d(p, s):
        for order in range(2):
            for dx, dy in A_ORDER:
                for core in range(2):
                    d_copy(p, s, order, core, dx, dy)[0].start()
            for core in range(2):
                copy, row, here = d_copy(p, s, order, core, 0, 0)

                @pl.when(jnp.logical_not(here))
                def _():
                    copy.start()

                @pl.when(here)
                def _():
                    out_ref[g, p, q] = z_send[p, row]

    def d_all(p, count):
        return pltpu.make_async_remote_copy(
            src_ref=z_send.at[p, pl.ds(0, count)],
            dst_ref=z_send.at[p, pl.ds(0, count)],
            send_sem=z_ssem.at[p, 0],
            recv_sem=b_rsem.at[p],
            device_id=(b, g),
            device_id_type=MESH,
        )

    mine = lax.rem(g + parity, 2)

    def pass_on(p, s):
        @pl.when(mine == s)
        def _():
            with jax.named_scope(f"wait_z#p={p}#s={s}"):
                wait_z(p)
            for dx, dy in A_ORDER:
                b_copy(p, dx, dy).start()
            out_ref[:, p, q] = z_recv[p, q]

    final = PHASES - 1
    steps = [(p, s) for p in range(PHASES) for s in range(2)]
    for k, (p, s) in enumerate(steps):
        combine(p, s)
        with jax.named_scope(f"send_z#p={p}#s={s}"):
            if p < final:
                send_z(p, s)
            else:
                send_d(p, s)
        if k >= LAG:
            pass_on(*steps[k - LAG])

    for p, s in steps:
        a_all(p, s).wait_send()
        own = in_class & ((mine == s) if p < final else (s == 0))
        part = CHIPS if p < final else 1

        @pl.when(own)
        def _():
            blocks(p, s, 4 * CHIPS - part).wait_send()

        @pl.when(jnp.logical_not(own))
        def _():
            blocks(p, s, 4 * CHIPS).wait_send()

    for p in range(1, PHASES):
        swap(p).wait_send()
    for p in range(final):
        with jax.named_scope(f"wait_b#p={p}"):
            b_all(p).wait_recv()
            b_all(p).wait_send()
    with jax.named_scope("wait_d"):

        @pl.when(in_class)
        def _():
            d_all(final, NZ * CHIPS - 1).wait_recv()

        @pl.when(jnp.logical_not(in_class))
        def _():
            d_all(final, NZ * CHIPS).wait_recv()


def on_device(band_coeffs, sign_table, slice_widths, owner_map):
    hbm = pl.BlockSpec(memory_space=pltpu.HBM)
    operands = (band_coeffs, sign_table, slice_widths.reshape(1, NSLICE), owner_map.reshape(1, NSLICE))
    operands = [pltpu.with_memory_space_constraint(v, pltpu.HBM) for v in operands]
    rows = pl.pallas_call(
        kernel,
        out_shape=jax.ShapeDtypeStruct((NZ, PHASES, CHIPS, TRI, 128), F32),
        in_specs=[hbm] * 4,
        out_specs=pl.BlockSpec(memory_space=pltpu.VMEM),
        scratch_shapes=[
            pltpu.VMEM((PHASES, BANDS, WIDE), F32),
            pltpu.VMEM((NPS, BANDS), jnp.int32),
            pltpu.VMEM((1, NSLICE), jnp.int32),
            pltpu.VMEM((1, NSLICE), jnp.int32),
            pltpu.VMEM((OUT, GROUPS * ROWS), BF16),
            pltpu.VMEM((OUT, GROUPS * ROWS), BF16),
            pltpu.VMEM((OUT, 128), F32),
            pltpu.VMEM((CHIPS, 4, USED, 128), F32),
            pltpu.VMEM((2, GROUPS, USED, 128), F32),
            pltpu.VMEM((PHASES - 1, CHIPS, 2, CHIP_USED, 128), F32),
            pltpu.VMEM((PHASES - 1, CHIPS, 2, CHIP_USED, 128), F32),
            pltpu.VMEM((PHASES - 1, CHIPS, 2, CHIP_USED, 128), F32),
            pltpu.VMEM((PHASES - 1, 2, CHIPS, CHIP_USED, 128), F32),
            pltpu.VMEM((PHASES, 2 * 4 * CHIPS, TRI, 128), F32),
            pltpu.VMEM((PHASES, CHIPS, NZ, TRI, 128), F32),
            pltpu.SemaphoreType.DMA((PHASES,)),
            pltpu.SemaphoreType.DMA((3,)),
            pltpu.SemaphoreType.DMA((PHASES, 2)),
            pltpu.SemaphoreType.DMA((PHASES, 2)),
            pltpu.SemaphoreType.DMA((PHASES - 1,)),
            pltpu.SemaphoreType.DMA((PHASES - 1,)),
            pltpu.SemaphoreType.DMA((PHASES, 2)),
            pltpu.SemaphoreType.DMA((PHASES,)),
            pltpu.SemaphoreType.DMA((2 * PHASES,)),
        ],
        compiler_params=pltpu.CompilerParams(
            collective_id=0, has_side_effects=True, vmem_limit_bytes=VMEM_LIMIT
        ),
        name="pseudobands",
    )(*operands)
    return jnp.transpose(rows.reshape(-1, TRI, 128), (1, 0, 2)).reshape(TRI, NZ * SLAB)


def solution(mesh):
    return jax.shard_map(
        on_device,
        mesh=mesh,
        in_specs=(P("band", "gslab"), P(None, "band"), P(), P()),
        out_specs=P(("band", "gslab"), None),
        check_vma=False,
    )
```
